32 devices in a mesh: dp: 4 (over y, core), tensor: 2 (over x), pipe: 4 (over z).
Axes of the slice: x: 2, y: 2, z: 4, core: 2. Of those that a mesh axis runs over, the one named last changes fastest.
Arguments:
- grad_parts: float32 [4, 4, 2, 64, 8192], P('dp', 'pipe', 'tensor'), may hold values from -24 to 24
- drop_flags: int32 [4, 4, 2, 64], P('dp', 'pipe', 'tensor'), may hold values from 0 to 1, as said below
- owner_order: int32 [4], replicated, may hold values from 0 to 3, each once
- step_count: int32 [], replicated, may hold values from 1 to 11
- master: float32 [4, 2, 64, 8192], P('pipe', 'tensor', None, 'dp'), may hold values from -6 to 6
- moment_m: float32 [4, 2, 64, 8192], P('pipe', 'tensor', None, 'dp'), may hold values from -0.15625 to 0.15625
- moment_v: float32 [4, 2, 64, 8192], P('pipe', 'tensor', None, 'dp'), may hold values from 0.0001 to 0.001
Outputs:
- new_master: float32 [4, 2, 64, 8192], P('pipe', 'tensor', None, 'dp')
- new_m: float32 [4, 2, 64, 8192], P('pipe', 'tensor', None, 'dp')
- new_v: float32 [4, 2, 64, 8192], P('pipe', 'tensor', None, 'dp')
- direction: float32 [4, 2, 64, 8192], P('pipe', 'tensor', None, 'dp')
- dropped_total: int32 [], replicated
The draws below stay inside these ranges and needn't reach their ends.
Inputs may be any that keep to these rules, and one draw needn't show every extreme that they name: `drop_flags`: A row may be flagged by every replica.
All inputs are finite; a program needn't handle non-finite values.
Results may differ from the reference program's by a relative error of at most 0.0003.
Values sent between devices are 32-bit elements; how exact they have to be, the bound alone decides.
A program may use at most 64 MiB of HBM per device.

```python
import math
import jax
import jax.numpy as jnp
from jax import lax

D = 8192
ROWS = 64
LAYERS = 4
SHARDS = 2
N_DP = 4


def draw_drop_flags(key, part):
    random_ones = jax.random.randint(jax.random.fold_in(key, 11), (N_DP, LAYERS, SHARDS, ROWS), 0, 4) == 0
    full_rows = jax.random.randint(jax.random.fold_in(key, 12), (LAYERS, SHARDS, ROWS), 0, 32) == 0
    forced = jax.random.randint(jax.random.fold_in(key, 13), (), 0, LAYERS * SHARDS * ROWS)
    position = jnp.arange(LAYERS * SHARDS * ROWS, dtype=jnp.int32).reshape(LAYERS, SHARDS, ROWS)
    every_replica = full_rows | (position == forced)
    return jnp.where(random_ones | every_replica[None], 1, 0).astype(jnp.int32)


def draw_grad_parts(key, part):
    block_cols = D // N_DP
    pairing = jax.random.permutation(jax.random.fold_in(key, 21), N_DP)
    column_block = jnp.arange(D, dtype=jnp.int32) // block_cols
    spiked = column_block[None, :] == pairing[:, None]
    factor = jnp.where(spiked, 4.0, 1.0).astype(jnp.float32)[:, None, None, None, :]
    noise = jax.random.normal(jax.random.fold_in(key, 22), (N_DP, LAYERS, SHARDS, ROWS, D), jnp.float32)
    own_part = jnp.clip(noise, -6.0, 6.0) * factor
    values = own_part
    return values.astype(jnp.float32)


def levels(own_key, dims, pieces, low, top_value):
    gain = 1.0
    for axis_at, shards_of in pieces:
        heights = jax.random.uniform(jax.random.fold_in(jax.random.fold_in(own_key, 6), axis_at), (shards_of,), jnp.float32, low / len(pieces), top_value / len(pieces))
        gain = gain * jnp.repeat(jnp.exp(heights), dims[axis_at] // shards_of).reshape((-1,) + (1,) * (len(dims) - 1 - axis_at))
    return gain


def gaussian(key, shape, spread, most, pieces=(), kind=jnp.bfloat16):
    array = jax.random.normal(key, shape, jnp.float32) * spread
    if len(pieces) > 0:
        array = levels(key, shape, pieces, -0.22, 0.18) * array
    return jnp.clip(array, min=-most, max=most).astype(kind)


def setup_inputs(seed: int = 0) -> dict:
    streams_of = jax.random.split(jax.random.key(seed), 8)
    return {
        "grad_parts": draw_grad_parts(jax.random.fold_in(streams_of[7], 71), 0),
        "drop_flags": draw_drop_flags(jax.random.fold_in(streams_of[7], 71), 0),
        "owner_order": jax.random.permutation(streams_of[2], N_DP).astype(jnp.int32),
        "step_count": jax.random.randint(streams_of[3], (), 1, 12).astype(jnp.int32),
        "master": gaussian(streams_of[4], (LAYERS, SHARDS, ROWS, D), 1.0, 6.0, ((0, 4), (1, 2), (3, 4)), jnp.float32),
        "moment_m": gaussian(streams_of[5], (LAYERS, SHARDS, ROWS, D), 0.01, 0.15625, ((0, 4), (1, 2), (3, 4)), jnp.float32),
        "moment_v": jnp.clip(jnp.exp(math.log(0.001) - 2.3025852 * jax.random.uniform(streams_of[6], (LAYERS, SHARDS, ROWS, D), jnp.float32) ** levels(streams_of[6], (LAYERS, SHARDS, ROWS, D), ((0, 4), (1, 2), (3, 4)), -0.2, 0.2)), 0.0001, 0.001),
    }


def reference(grad_parts, drop_flags, owner_order, step_count, master, moment_m, moment_v):
    kept = (1 - drop_flags).astype(jnp.float32)

    def accumulate(carry, pair):
        part, keep = pair
        return ((carry[0] + part * keep[..., None], carry[1] + keep), None)
    start = (jnp.zeros(grad_parts.shape[1:], jnp.float32), jnp.zeros(kept.shape[1:], jnp.float32))
    (total, count), unused = lax.scan(accumulate, start, (grad_parts, kept))
    mean_grad = total / jnp.maximum(count, 1.0)[..., None]
    shape = mean_grad.shape
    blocks = mean_grad.reshape(shape[0], shape[1], shape[2], N_DP, shape[3] // N_DP)
    grad = jnp.take(blocks, owner_order, axis=3).reshape(shape)
    entries = shape[0] * shape[1] * shape[2] * shape[3]
    rms = jnp.sqrt(jnp.sum(grad * grad) / entries)
    clip = jnp.minimum(1.0, 0.05 / (rms + 1e-06))
    scaled = clip * grad
    new_m = 0.9 * moment_m + 0.1 * scaled
    new_v = 0.999 * moment_v + 0.001 * scaled * scaled
    steps = step_count.astype(jnp.float32)
    m_hat = new_m / (1.0 - jnp.power(0.9, steps))
    v_hat = new_v / (1.0 - jnp.power(0.999, steps))
    direction = m_hat / (jnp.sqrt(v_hat) + 1e-08) + 0.1 * master
    new_master = master - 0.001 * direction
    dropped_total = jnp.sum(drop_flags).astype(jnp.int32)
    return (new_master, new_m, new_v, direction, dropped_total)
```

```python
import functools
import itertools
import jax
import jax.numpy as jnp
from jax import lax
from jax.experimental import pallas as pl
from jax.experimental.pallas import tpu as pltpu
from jax.sharding import PartitionSpec as P

AXES = ("dp", "tensor", "pipe")
MESH = pl.DeviceIdType.MESH
LANES = 128
SUBLANES = 8
DIRECT = 64


def as_column(row, rows):
    square = (rows, rows)
    diagonal = lax.broadcasted_iota(jnp.int32, square, 0) == lax.broadcasted_iota(jnp.int32, square, 1)
    return jnp.sum(jnp.where(diagonal, jnp.broadcast_to(row, square), 0.0), axis=1, keepdims=True)


def int_power(base, exponent):
    result = jnp.ones(exponent.shape, jnp.float32)
    square = jnp.full(exponent.shape, base, jnp.float32)
    for bit in range(31):
        result = jnp.where((exponent >> bit) & 1 == 1, result * square, result)
        square = square * square
    return result


def exchange(
    sizes, stages, cuts,
    order_hbm, flags_hbm, grad_hbm, w_hbm, m_hbm, v_hbm,
    total, w_vmem, m_vmem, v_vmem, stats,
    order_ref, flags_ref, g_bufs, pair_send, pair_recv, ring_send, ring_recv,
    kept_send, kept_recv, red_sends, red_recvs,
    o_sem, g_sem, w_sem, ps_sem, pr_sem, rs_sem, rr_sem, k_sem, a_sem, ready_sem,
):
    n = sizes["dp"]
    chips = n // 2
    rows, width = total.shape
    parts = [(start, end - start) for start, end in zip(cuts, cuts[1:])]
    me = {axis: lax.axis_index(axis) for axis in AXES}
    chip, core = lax.div(me["dp"], 2), lax.rem(me["dp"], 2)

    def peer(offsets):
        return {axis: lax.rem(me[axis] + off, sizes[axis]) for axis, off in offsets.items()}

    def offsets_of(axes):
        ranges = [range(sizes[axis]) for axis in axes]
        return [dict(zip(axes, offs)) for offs in itertools.product(*ranges) if any(offs)]

    small = [
        pltpu.make_async_copy(flags_hbm, flags_ref, o_sem.at[0]),
        pltpu.make_async_copy(order_hbm, order_ref, o_sem.at[1]),
    ]
    for copy in small:
        copy.start()
    loads = []
    for k, (start, size) in enumerate(parts):
        for b in range(n):
            pltpu.make_async_copy(
                grad_hbm.at[0, 0, 0, pl.ds(start, size), pl.ds(b * width, width)], g_bufs[k].at[b], g_sem.at[k]
            ).start()
        loads.append(pltpu.make_async_copy(g_bufs[k], g_bufs[k], g_sem.at[k]))

    def greet(sem, axis):
        if axis == "dp":
            for off in range(1, n):
                pl.semaphore_signal(sem, inc=1, device_id=peer({"dp": off}), device_id_type=MESH)
            return n - 1
        at, last = me[axis], sizes[axis] - 1

        @pl.when(at > 0)
        def _():
            pl.semaphore_signal(sem, inc=1, device_id={axis: at - 1}, device_id_type=MESH)

        @pl.when(at < last)
        def _():
            pl.semaphore_signal(sem, inc=1, device_id={axis: at + 1}, device_id_type=MESH)

        return jnp.minimum(at, 1) + jnp.minimum(last - at, 1)

    barrier = pltpu.get_barrier_semaphore()
    met = sum(greet(barrier, axis) for axis in AXES)
    rounds = ["pipe"] * max(sizes["pipe"] - 2, 0) + ["tensor"] * (sizes["tensor"] - 1) + ["dp"]
    left, owed = list(rounds), []

    def next_round():
        if owed:
            at, amount = owed.pop()
            pl.semaphore_wait(ready_sem.at[at], amount)
        if left:
            at = len(rounds) - len(left)
            owed.append((at, greet(ready_sem.at[at], left.pop(0))))

    for copy in small:
        copy.wait()
    flags_row = flags_ref[0].astype(jnp.float32)
    kept_row = 1.0 - flags_row
    kept = as_column(kept_row, rows)
    kept_send[0, :, 0:rows] = kept_row
    dropped = jnp.sum(flags_row, axis=1, keepdims=True)

    def chip_at(slot):
        return lax.rem(chip + slot, chips)

    def term(k, owner):
        start, size = parts[k]
        return g_bufs[k][order_ref[owner]] * kept[start:start + size]

    def rows_of(ref, slot, k):
        start, size = parts[k]
        return ref.at[slot, pl.ds(start, size)]

    sibling = {"dp": chip * 2 + 1 - core}
    pair = {}

    def send_pair(k, slot):
        copy = pltpu.make_async_remote_copy(
            rows_of(pair_send, slot, k), rows_of(pair_recv, slot, k),
            ps_sem.at[0], pr_sem.at[k if slot else len(parts)],
            device_id=sibling, device_id_type=MESH,
        )
        copy.start()
        pair[k, slot] = copy

    far = list(range(1, chips))
    for k, (start, size) in enumerate(parts):
        with jax.named_scope(f"load_wait{k}"):
            loads[k].wait()
        for slot in far:
            pair_send[slot, start:start + size, :] = term(k, chip_at(slot) * 2 + 1 - core)
        if k == 0:
            with jax.named_scope("barrier_wait"):
                pl.semaphore_wait(barrier, met)
        for slot in far:
            send_pair(k, slot)
        if k == 0:
            for off in range(1, n):
                pltpu.make_async_remote_copy(
                    kept_send.at[0], kept_recv.at[off - 1], k_sem.at[0], k_sem.at[1],
                    device_id=peer({"dp": off}), device_id_type=MESH,
                ).start()
    kepts = pltpu.make_async_remote_copy(
        kept_recv, kept_recv, k_sem.at[0], k_sem.at[1], device_id=sibling, device_id_type=MESH
    )

    ring = {}
    for k, (start, size) in enumerate(parts):
        for slot in far:
            target = chip_at(slot) * 2 + core
            mine = term(k, target)
            with jax.named_scope(f"pair_wait{k}"):
                if slot == far[0]:
                    pltpu.make_async_remote_copy(
                        pair_recv.at[pl.ds(1, chips - 1), pl.ds(start, size)],
                        pair_recv.at[pl.ds(1, chips - 1), pl.ds(start, size)],
                        ps_sem.at[0], pr_sem.at[k], device_id=sibling, device_id_type=MESH,
                    ).wait_recv()
            ring_send[slot - 1, start:start + size, :] = pair_recv[slot, start:start + size, :] + mine
            copy = pltpu.make_async_remote_copy(
                rows_of(ring_send, slot - 1, k), rows_of(ring_recv, slot - 1, k),
                rs_sem.at[0], rr_sem.at[k, slot - 1],
                device_id={"dp": target}, device_id_type=MESH,
            )
            copy.start()
            ring[k, slot] = copy

    next_round()
    for k, (start, size) in enumerate(parts):
        pair_send[0, start:start + size, :] = term(k, chip * 2 + 1 - core)
        send_pair(k, 0)
    with jax.named_scope("kept_wait"):
        kepts.wait_recv()
    count_row = kept_row
    for i in range(n - 1):
        count_row = count_row + kept_recv[i, :, 0:rows]
    inverse = 1.0 / jnp.maximum(as_column(count_row, rows), 1.0)
    states = []
    for i, (source, target) in enumerate(((w_hbm, w_vmem), (m_hbm, m_vmem), (v_hbm, v_vmem))):
        copy = pltpu.make_async_copy(source.at[0, 0], target, w_sem.at[i])
        copy.start()
        states.append(copy)

    pltpu.make_async_remote_copy(
        pair_recv.at[0], pair_recv.at[0], ps_sem.at[0], pr_sem.at[len(parts)],
        device_id=sibling, device_id_type=MESH,
    ).wait_recv()
    for k, (start, size) in enumerate(parts):
        total[start:start + size, :] = pair_recv[0, start:start + size, :] + term(k, me["dp"])
    for copy in states:
        copy.wait()

    per_part = -(-(len(rounds) + 1) // max(len(parts) - 1, 1))
    squares = jnp.zeros((SUBLANES, LANES), jnp.float32)
    for k, (start, size) in enumerate(parts):
        at = slice(start, start + size)
        value = total[at, :]
        for slot in far:
            with jax.named_scope(f"ring_wait{k}"):
                ring[k, slot].wait_recv()
            value = value + ring_recv[slot - 1, at, :]
        value = value * inverse[at]
        total[at, :] = value
        squares = squares + jnp.sum(
            (value * value).reshape(size // SUBLANES, SUBLANES, width // LANES, LANES), axis=(0, 2)
        )
        for _ in range(per_part):
            next_round()

    result = [jnp.sum(squares, axis=0, keepdims=True), jnp.broadcast_to(dropped, (1, LANES))]
    done = []
    for stage, (axes, send, recv) in enumerate(zip(stages, red_sends, red_recvs)):
        for i, row in enumerate(result):
            send[i:i + 1, :] = row
        with jax.named_scope("norm_send"):
            for i, off in enumerate(offsets_of(axes)):
                pltpu.make_async_remote_copy(
                    send, recv.at[i], a_sem.at[stage, 0], a_sem.at[stage, 1],
                    device_id=peer(off), device_id_type=MESH,
                ).start()
        copy = pltpu.make_async_remote_copy(
            recv, recv, a_sem.at[stage, 0], a_sem.at[stage, 1], device_id=sibling, device_id_type=MESH
        )
        done.append(copy)
        with jax.named_scope("norm_wait"):
            copy.wait_recv()
        for i in range(len(offsets_of(axes))):
            result = [row + recv[i, j:j + 1, :] for j, row in enumerate(result)]
    for i, row in enumerate(result):
        stats[i:i + 1, :] = row
    stats[2:8, :] = jnp.zeros((6, LANES), jnp.float32)

    with jax.named_scope("send_wait"):
        pltpu.make_async_remote_copy(
            pair_send, pair_recv, ps_sem.at[0], pr_sem.at[0], device_id=sibling, device_id_type=MESH
        ).wait_send()
        kepts.wait_send()
        if far:
            pltpu.make_async_remote_copy(
                ring_send, ring_recv, rs_sem.at[0], rr_sem.at[0, 0], device_id=sibling, device_id_type=MESH
            ).wait_send()
        for copy in done:
            copy.wait_send()


def update(
    entries, chunks, step_ref, stats, grad_ref, w_ref, m_ref, v_ref,
    w_out, m_out, v_out, dir_out, drop_out, bufs, drop_ref, sems,
):
    rows, width = grad_ref.shape
    part = rows // chunks
    steps = jnp.full((SUBLANES, LANES), step_ref[...], jnp.int32)
    scale_m = (1.0 / (1.0 - int_power(0.9, steps)))[0:1, 0:1]
    scale_v = (1.0 / (1.0 - int_power(0.999, steps)))[0:1, 0:1]
    summed = jnp.sum(jnp.broadcast_to(stats[0:1, :], (SUBLANES, LANES)), axis=1, keepdims=True)
    rms = jnp.sqrt(summed * (1.0 / entries))[0:1]
    clip = jnp.minimum(1.0, 0.05 / (rms + 1e-06))
    outs = (w_out, m_out, v_out, dir_out)
    for k in range(chunks):
        at = slice(k * part, (k + 1) * part)
        scaled = grad_ref[at, :] * clip
        new_m = 0.9 * m_ref[at, :] + 0.1 * scaled
        new_v = 0.999 * v_ref[at, :] + 0.001 * (scaled * scaled)
        weights = w_ref[at, :]
        direction = (new_m * scale_m) / (jnp.sqrt(new_v * scale_v) + 1e-08) + 0.1 * weights
        values = (weights - 0.001 * direction, new_m, new_v, direction)
        for i, (value, out) in enumerate(zip(values, outs)):
            bufs[i, at, :] = value
            pltpu.make_async_copy(bufs.at[i, pl.ds(k * part, part)], out.at[0, 0, pl.ds(k * part, part)], sems.at[i]).start()
        if k == 0:
            drop_ref[0] = jnp.max(stats[1:2, :]).astype(jnp.int32)
            drop = pltpu.make_async_copy(drop_ref, drop_out, sems.at[4])
            drop.start()
    for i, out in enumerate(outs):
        pltpu.make_async_copy(bufs.at[i], out.at[0, 0], sems.at[i]).wait()
    drop.wait()


def body(sizes, grad_parts, drop_flags, owner_order, step_count, master, moment_m, moment_v):
    n = sizes["dp"]
    chips = n // 2
    rows, columns = grad_parts.shape[-2:]
    width = master.shape[-1]
    chunks = rows // 8
    cuts = sorted({0, 8, rows // 2, rows - 8, rows})
    devices = n * sizes["tensor"] * sizes["pipe"]
    stages = [AXES] if devices <= DIRECT else [(axis,) for axis in AXES]
    peers = []
    for axes in stages:
        size = 1
        for axis in axes:
            size *= sizes[axis]
        peers.append(size - 1)
    entries = rows * columns * sizes["tensor"] * sizes["pipe"]
    padded = -(-rows // LANES) * LANES
    others = max(chips - 1, 1)
    rounds = max(sizes["pipe"] - 2, 0) + sizes["tensor"]
    f32 = jnp.float32
    dma = pltpu.SemaphoreType.DMA
    vmem = pl.BlockSpec(memory_space=pltpu.VMEM)
    smem = pl.BlockSpec(memory_space=pltpu.SMEM)
    hbm = pl.BlockSpec(memory_space=pltpu.HBM)
    state = jax.ShapeDtypeStruct(master.shape, f32)
    held = pltpu.VMEM((rows, width), f32)
    block = rows * columns * 4
    inputs = (owner_order, drop_flags.reshape(drop_flags.shape[-3:]), grad_parts, master, moment_m, moment_v)
    total, weights, first, second, stats = pl.pallas_call(
        functools.partial(exchange, sizes, stages, cuts),
        out_shape=(held, held, held, held, pltpu.VMEM((SUBLANES, LANES), f32)),
        in_specs=[hbm] * 6,
        out_specs=(vmem,) * 5,
        scratch_shapes=[
            pltpu.SMEM((n,), jnp.int32),
            pltpu.VMEM((1, 1, rows), jnp.int32),
            [pltpu.VMEM((n, end - start, width), f32) for start, end in zip(cuts, cuts[1:])],
            pltpu.VMEM((chips, rows, width), f32),
            pltpu.VMEM((chips, rows, width), f32),
            pltpu.VMEM((others, rows, width), f32),
            pltpu.VMEM((others, rows, width), f32),
            pltpu.VMEM((1, 1, padded), f32),
            pltpu.VMEM((n - 1, 1, padded), f32),
            [pltpu.VMEM((2, LANES), f32) for _ in peers],
            [pltpu.VMEM((max(size, 1), 2, LANES), f32) for size in peers],
            dma((2,)),
            dma((len(cuts) - 1,)),
            dma((3,)),
            dma((1,)),
            dma((len(cuts),)),
            dma((1,)),
            dma((len(cuts) - 1, others)),
            dma((2,)),
            dma((len(peers), 2)),
            pltpu.SemaphoreType.REGULAR((rounds,)),
        ],
        compiler_params=pltpu.CompilerParams(
            collective_id=0, has_side_effects=True, vmem_limit_bytes=8 * block
        ),
        cost_estimate=pl.CostEstimate(
            flops=8 * rows * columns, bytes_accessed=20 * rows * columns * 4, transcendentals=0
        ),
    )(*(pltpu.with_memory_space_constraint(x, pltpu.HBM) for x in inputs))
    outs = pl.pallas_call(
        functools.partial(update, entries, chunks),
        out_shape=(state, state, state, state, jax.ShapeDtypeStruct((1,), jnp.int32)),
        in_specs=[smem] + [vmem] * 5,
        out_specs=(hbm,) * 5,
        scratch_shapes=[pltpu.VMEM((4, rows, width), f32), pltpu.SMEM((1,), jnp.int32), dma((5,))],
        compiler_params=pltpu.CompilerParams(vmem_limit_bytes=8 * block),
        cost_estimate=pl.CostEstimate(
            flops=20 * rows * width, bytes_accessed=8 * rows * width * 4, transcendentals=0
        ),
    )(step_count, stats, total, weights, first, second)
    return (*outs[:4], outs[4].reshape(()))


def solution(mesh):
    return jax.shard_map(
        functools.partial(body, dict(mesh.shape)),
        mesh=mesh,
        in_specs=(
            P("dp", "pipe", "tensor", None, None),
            P("dp", "pipe", "tensor", None),
            P(),
            P(),
            P("pipe", "tensor", None, "dp"),
            P("pipe", "tensor", None, "dp"),
            P("pipe", "tensor", None, "dp"),
        ),
        out_specs=(
            P("pipe", "tensor", None, "dp"),
            P("pipe", "tensor", None, "dp"),
            P("pipe", "tensor", None, "dp"),
            P("pipe", "tensor", None, "dp"),
            P(),
        ),
        check_vma=False,
    )
```

```python
import functools
import itertools
import math
import jax
import jax.numpy as jnp
from jax import lax
from jax.experimental import pallas as pl
from jax.experimental.pallas import tpu as pltpu
from jax.sharding import PartitionSpec as P

AXES = ("dp", "tensor", "pipe")
MESH = pl.DeviceIdType.MESH
LANES = 128
SUBLANES = 8
DIRECT = 64
PIECES = 4


def as_column(row, rows):
    square = (rows, rows)
    diagonal = lax.broadcasted_iota(jnp.int32, square, 0) == lax.broadcasted_iota(jnp.int32, square, 1)
    return jnp.sum(jnp.where(diagonal, jnp.broadcast_to(row, square), 0.0), axis=1, keepdims=True)


def int_power(base, exponent):
    result = jnp.ones(exponent.shape, jnp.float32)
    square = jnp.full(exponent.shape, base, jnp.float32)
    for bit in range(31):
        result = jnp.where((exponent >> bit) & 1 == 1, result * square, result)
        square = square * square
    return result


def can_relay(sizes, stages):
    return sizes["dp"] == 4 and sizes["tensor"] == 2 and len(stages) == 1 and sizes["pipe"] > 1


def exchange(
    sizes, stages, cuts,
    step_ref, order_hbm, flags_hbm, grad_hbm, w_hbm, m_hbm, v_hbm,
    total, held, stats,
    order_ref, flags_ref, g_bufs, pair_send, pair_recv, ring_send, ring_recv,
    kept_send, kept_recv, red_sends, red_recvs,
    relay_buf, o_sem, g_sem, w_sem, ps_sem, pr_sem, rs_sem, rr_sem, k_sem, a_sem, via_sem, chain_sem, ready_sem,
):
    n = sizes["dp"]
    chips = n // 2
    relayed = can_relay(sizes, stages)
    rows, width = total.shape
    parts = [(start, end - start) for start, end in zip(cuts, cuts[1:])]
    me = {axis: lax.axis_index(axis) for axis in AXES}
    chip, core = lax.div(me["dp"], 2), lax.rem(me["dp"], 2)

    def peer(offsets):
        return {axis: lax.rem(me[axis] + off, sizes[axis]) for axis, off in offsets.items()}

    def offsets_of(axes):
        ranges = [range(sizes[axis]) for axis in axes]
        return [dict(zip(axes, offs)) for offs in itertools.product(*ranges) if any(offs)]

    small = [
        pltpu.make_async_copy(flags_hbm, flags_ref, o_sem.at[0]),
        pltpu.make_async_copy(order_hbm, order_ref, o_sem.at[1]),
    ]
    for copy in small:
        copy.start()
    loads = []

    def load(k):
        start, size = parts[k]
        for b in range(n):
            pltpu.make_async_copy(
                grad_hbm.at[0, 0, 0, pl.ds(start, size), pl.ds(b * width, width)], g_bufs[k].at[b], g_sem.at[k]
            ).start()
        loads.append(pltpu.make_async_copy(g_bufs[k], g_bufs[k], g_sem.at[k]))

    load(0)

    def greet(sem, axis):
        if axis == "dp":
            for off in range(1, n):
                pl.semaphore_signal(sem, inc=1, device_id=peer({"dp": off}), device_id_type=MESH)
            return n - 1
        at, last = me[axis], sizes[axis] - 1

        @pl.when(at > 0)
        def _():
            pl.semaphore_signal(sem, inc=1, device_id={**home, axis: at - 1}, device_id_type=MESH)

        @pl.when(at < last)
        def _():
            pl.semaphore_signal(sem, inc=1, device_id={**home, axis: at + 1}, device_id_type=MESH)

        return jnp.minimum(at, 1) + jnp.minimum(last - at, 1)

    sibling = {"dp": chip * 2 + 1 - core}
    barrier = pltpu.get_barrier_semaphore()

    @pl.when(core == 1)
    def _():
        pl.semaphore_signal(barrier, inc=1, device_id=sibling, device_id_type=MESH)

    home = {"dp": chip * 2 + 1}
    for off in range(1, chips):
        pl.semaphore_signal(
            barrier, inc=1, device_id={"dp": lax.rem(chip + off, chips) * 2 + 1}, device_id_type=MESH
        )
    met = 2 * (chips - 1 + greet(barrier, "tensor") + greet(barrier, "pipe"))
    home = {}
    rounds = ["pipe"] * max(sizes["pipe"] - 2, 0) + ["tensor"] * (sizes["tensor"] - 1) + ["dp"]
    left, owed = list(rounds), []

    def next_round():
        if owed:
            at, amount = owed.pop()
            pl.semaphore_wait(ready_sem.at[at], amount)
        if left:
            at = len(rounds) - len(left)
            owed.append((at, greet(ready_sem.at[at], left.pop(0))))

    load(1)

    @pl.when(core == 0)
    def _():
        pl.semaphore_wait(barrier, 1)
        pl.semaphore_signal(chain_sem.at[2], inc=1, device_id=sibling, device_id_type=MESH)

    for copy in small:
        copy.wait()
    for k in range(2, len(parts)):
        load(k)
    flags_row = flags_ref[0].astype(jnp.float32)
    kept_row = 1.0 - flags_row
    kept = as_column(kept_row, rows)
    kept_send[0, :, 0:rows] = kept_row
    dropped = jnp.sum(flags_row, axis=1, keepdims=True)

    def chip_at(slot):
        return lax.rem(chip + slot, chips)

    def term(k, owner):
        start, size = parts[k]
        return g_bufs[k][order_ref[owner]] * kept[start:start + size]

    def rows_of(ref, slot, k):
        start, size = parts[k]
        return ref.at[slot, pl.ds(start, size)]

    pair = {}

    def send_pair(k, slot):
        copy = pltpu.make_async_remote_copy(
            rows_of(pair_send, slot, k), rows_of(pair_recv, slot, k),
            ps_sem.at[0], pr_sem.at[k if slot else len(parts)],
            device_id=sibling, device_id_type=MESH,
        )
        copy.start()
        pair[k, slot] = copy

    far = list(range(1, chips))
    def to_sibling(k):
        start, size = parts[k]
        with jax.named_scope(f"load_wait{k}"):
            loads[k].wait()
        for slot in far:
            pair_send[slot, start:start + size, :] = term(k, chip_at(slot) * 2 + 1 - core)
        if k == 0:
            with jax.named_scope("sibling_wait"):
                @pl.when(core == 1)
                def _():
                    pl.semaphore_wait(chain_sem.at[2], 1)
        for slot in far:
            send_pair(k, slot)

    kepts = pltpu.make_async_remote_copy(
        kept_recv, kept_recv, k_sem.at[0], k_sem.at[1], device_id=sibling, device_id_type=MESH
    )

    ring = {}
    swing = len(parts) - 2
    far_end = sizes["pipe"] - 1
    gap = 2 * me["pipe"] - far_end
    across = {"dp": chip_at(1) * 2 + core}
    direct = [k for k in range(len(parts)) if k != swing]
    lend = [gap >= 1, gap >= 3, 2 * me["tensor"] >= sizes["tensor"]] if relayed else []
    borrow = [gap <= -1, gap <= -3, 2 * me["tensor"] < sizes["tensor"]] if relayed else []
    mirror = [{"pipe": far_end - me["pipe"]}] * 2 + [{"tensor": sizes["tensor"] - 1 - me["tensor"]}]
    quarter = width // PIECES

    def piece(ref, h):
        start, size = parts[swing]
        return ref.at[0, pl.ds(start, size), pl.ds(h * quarter, quarter)]

    def swing_copy(h):
        return pltpu.make_async_remote_copy(
            piece(ring_send, h), piece(ring_recv, h), rs_sem.at[0], rr_sem.at[swing, 0],
            device_id=across, device_id_type=MESH,
        )

    def via_copy(h):
        return pltpu.make_async_remote_copy(
            piece(ring_send, h), relay_buf.at[h], rs_sem.at[0], via_sem.at[h],
            device_id={**across, **mirror[h]}, device_id_type=MESH,
        )

    def forward_copy(h):
        return pltpu.make_async_remote_copy(
            relay_buf.at[h], piece(ring_recv, h), via_sem.at[h], rr_sem.at[swing, 0],
            device_id=mirror[h], device_id_type=MESH,
        )

    def climb():
        at = me["pipe"]

        @pl.when(at >= 2)
        def _():
            pl.semaphore_wait(chain_sem.at[0], 1)

        @pl.when((at >= 1) & (at < far_end))
        def _():
            pl.semaphore_signal(chain_sem.at[0], inc=1, device_id={"pipe": at + 1}, device_id_type=MESH)

        @pl.when(lend[0] | lend[2])
        def _():
            pl.semaphore_signal(chain_sem.at[1], inc=1, device_id=across, device_id_type=MESH)

    def to_owner(k):
        start, size = parts[k]
        for slot in far:
            target = chip_at(slot) * 2 + core
            mine = term(k, target)
            with jax.named_scope(f"pair_wait{k}"):
                if slot == far[0]:
                    pltpu.make_async_remote_copy(
                        pair_recv.at[pl.ds(1, chips - 1), pl.ds(start, size)],
                        pair_recv.at[pl.ds(1, chips - 1), pl.ds(start, size)],
                        ps_sem.at[0], pr_sem.at[k], device_id=sibling, device_id_type=MESH,
                    ).wait_recv()
            ring_send[slot - 1, start:start + size, :] = pair_recv[slot, start:start + size, :] + mine
            if relayed and k == swing:
                @pl.when(lend[0] | lend[2])
                def _():
                    with jax.named_scope("chain_wait"):
                        pl.semaphore_wait(chain_sem.at[1], 1)

                for h, away in enumerate(lend):
                    @pl.when(away)
                    def _():
                        via_copy(h).start()

                for h, away in enumerate(lend):
                    @pl.when(jnp.logical_not(away))
                    def _():
                        swing_copy(h).start()
                for h in range(len(lend), PIECES):
                    swing_copy(h).start()
                continue
            copy = pltpu.make_async_remote_copy(
                rows_of(ring_send, slot - 1, k), rows_of(ring_recv, slot - 1, k),
                rs_sem.at[0], rr_sem.at[k, slot - 1],
                device_id={"dp": target}, device_id_type=MESH,
            )
            copy.start()
            ring[k, slot] = copy

    to_sibling(0)
    to_sibling(1)
    with jax.named_scope("barrier_wait"):
        @pl.when(core == 1)
        def _():
            pl.semaphore_wait(barrier, met)
            pl.semaphore_signal(chain_sem.at[2], inc=1, device_id=sibling, device_id_type=MESH)

        @pl.when(core == 0)
        def _():
            pl.semaphore_wait(chain_sem.at[2], 1)
    for off in range(1, n):
        pltpu.make_async_remote_copy(
            kept_send.at[0], kept_recv.at[off - 1], k_sem.at[0], k_sem.at[1],
            device_id=peer({"dp": off}), device_id_type=MESH,
        ).start()
    to_owner(0)
    if relayed:
        climb()
    to_owner(1)
    for k in range(2, len(parts)):
        to_sibling(k)
    for k in direct[2:] + [swing]:
        to_owner(k)

    next_round()
    for k, (start, size) in enumerate(parts):
        pair_send[0, start:start + size, :] = term(k, chip * 2 + 1 - core)
        send_pair(k, 0)
    with jax.named_scope("kept_wait"):
        kepts.wait_recv()
    count_row = kept_row
    for i in range(n - 1):
        count_row = count_row + kept_recv[i, :, 0:rows]
    inverse = 1.0 / jnp.maximum(as_column(count_row, rows), 1.0)
    for i, source in enumerate((w_hbm, m_hbm, v_hbm)):
        pltpu.make_async_copy(source.at[0, 0], held.at[i], w_sem.at[0]).start()

    pltpu.make_async_remote_copy(
        pair_recv.at[0], pair_recv.at[0], ps_sem.at[0], pr_sem.at[len(parts)],
        device_id=sibling, device_id_type=MESH,
    ).wait_recv()
    for k, (start, size) in enumerate(parts):
        total[start:start + size, :] = pair_recv[0, start:start + size, :] + term(k, me["dp"])
    pltpu.make_async_copy(held, held, w_sem.at[0]).wait()
    held[1] = 0.9 * held[1]
    held[2] = 0.999 * held[2]
    steps = jnp.full((SUBLANES, LANES), step_ref[...], jnp.int32)
    stats[0:8, :] = jnp.zeros((SUBLANES, LANES), jnp.float32)
    stats[8:16, :] = 1.0 / (1.0 - int_power(0.9, steps))
    stats[16:24, :] = 1.0 / (1.0 - int_power(0.999, steps))

    if relayed:
        for h in (2, 0, 1):
            @pl.when(borrow[h])
            def _():
                with jax.named_scope(f"relay_wait{h}"):
                    via_copy(h).wait_recv()
                forward_copy(h).start()

    per_part = -(-(len(rounds) + 1) // max(len(parts) - 1, 1))
    squares = jnp.zeros((SUBLANES, LANES), jnp.float32)
    for k, (start, size) in enumerate(parts):
        at = slice(start, start + size)
        value = total[at, :]
        for slot in far:
            with jax.named_scope(f"ring_wait{k}"):
                if relayed and k == swing:
                    pltpu.make_async_remote_copy(
                        ring_recv.at[0, pl.ds(start, size)], ring_recv.at[0, pl.ds(start, size)],
                        rs_sem.at[0], rr_sem.at[swing, 0], device_id=across, device_id_type=MESH,
                    ).wait_recv()
                else:
                    ring[k, slot].wait_recv()
            value = value + ring_recv[slot - 1, at, :]
        value = value * inverse[at]
        total[at, :] = value
        squares = squares + jnp.sum(
            (value * value).reshape(size // SUBLANES, SUBLANES, width // LANES, LANES), axis=(0, 2)
        )
        for _ in range(per_part):
            next_round()

    result = [jnp.sum(squares, axis=0, keepdims=True), jnp.broadcast_to(dropped, (1, LANES))]
    done = []
    for stage, (axes, send, recv) in enumerate(zip(stages, red_sends, red_recvs)):
        for i, row in enumerate(result):
            send[i:i + 1, :] = row
        with jax.named_scope("norm_send"):
            back, stride = 0, 1
            for axis in reversed(axes):
                back, stride = back + lax.rem(sizes[axis] - me[axis], sizes[axis]) * stride, stride * sizes[axis]

            def share(i, device):
                pltpu.make_async_remote_copy(
                    send, recv.at[i], a_sem.at[stage, 0], a_sem.at[stage, 1],
                    device_id=device, device_id_type=MESH,
                ).start()

            @pl.when(back > 0)
            def _():
                share(back - 1, dict.fromkeys(axes, 0))

            for i, off in enumerate(offsets_of(axes)):
                @pl.when(back != i + 1)
                def _():
                    share(i, peer(off))
        copy = pltpu.make_async_remote_copy(
            recv, recv, a_sem.at[stage, 0], a_sem.at[stage, 1], device_id=sibling, device_id_type=MESH
        )
        done.append(copy)
        with jax.named_scope("norm_wait"):
            copy.wait_recv()
        for i in range(len(offsets_of(axes))):
            result = [row + recv[i, j:j + 1, :] for j, row in enumerate(result)]
    for i, row in enumerate(result):
        stats[i:i + 1, :] = row

    with jax.named_scope("send_wait"):
        pltpu.make_async_remote_copy(
            pair_send, pair_recv, ps_sem.at[0], pr_sem.at[0], device_id=sibling, device_id_type=MESH
        ).wait_send()
        kepts.wait_send()
        if far:
            pltpu.make_async_remote_copy(
                ring_send, ring_recv, rs_sem.at[0], rr_sem.at[0, 0], device_id=sibling, device_id_type=MESH
            ).wait_send()
        for copy in done:
            copy.wait_send()
        if relayed:
            for h, taken in enumerate(borrow):
                @pl.when(taken)
                def _():
                    forward_copy(h).wait_send()


def update(
    entries, chunks, stats, grad_ref, held,
    w_out, m_out, v_out, dir_out, drop_out, bufs, drop_ref, sems,
):
    rows, width = grad_ref.shape
    part = rows // chunks
    scale_m = jnp.concatenate([stats[8:16, :]] * (width // LANES), axis=1)
    scale_v = jnp.concatenate([stats[16:24, :]] * (width // LANES), axis=1)
    summed = jnp.sum(jnp.broadcast_to(stats[0:1, :], (SUBLANES, LANES)), axis=1, keepdims=True)
    rms = jnp.sqrt(summed * (1.0 / entries))
    clip = jnp.minimum(1.0, 0.05 / (rms + 1e-06))
    share_m, share_v = 0.1 * clip, math.sqrt(0.001) * clip
    outs = (w_out, m_out, v_out, dir_out)
    for k in range(chunks):
        at = slice(k * part, (k + 1) * part)
        grad = grad_ref[at, :]
        root = grad * share_v
        new_m = held[1, at, :] + grad * share_m
        new_v = held[2, at, :] + root * root
        weights = held[0, at, :]
        corrected = new_v * scale_v
        direction = (new_m * scale_m) / (corrected * lax.rsqrt(corrected) + 1e-08) + 0.1 * weights
        values = (weights - 0.001 * direction, new_m, new_v, direction)
        for i, (value, out) in enumerate(zip(values, outs)):
            bufs[i, at, :] = value
            pltpu.make_async_copy(bufs.at[i, pl.ds(k * part, part)], out.at[0, 0, pl.ds(k * part, part)], sems.at[i]).start()
        if k == 0:
            drop_ref[0] = jnp.max(stats[1:2, :]).astype(jnp.int32)
            drop = pltpu.make_async_copy(drop_ref, drop_out, sems.at[4])
            drop.start()
    for i, out in enumerate(outs):
        pltpu.make_async_copy(bufs.at[i], out.at[0, 0], sems.at[i]).wait()
    drop.wait()


def body(sizes, grad_parts, drop_flags, owner_order, step_count, master, moment_m, moment_v):
    n = sizes["dp"]
    chips = n // 2
    rows, columns = grad_parts.shape[-2:]
    width = master.shape[-1]
    chunks = rows // 8
    cuts = sorted({0, 8, rows - 24, rows - 8, rows})
    devices = n * sizes["tensor"] * sizes["pipe"]
    stages = [AXES] if devices <= DIRECT else [(axis,) for axis in AXES]
    peers = []
    for axes in stages:
        size = 1
        for axis in axes:
            size *= sizes[axis]
        peers.append(size - 1)
    entries = rows * columns * sizes["tensor"] * sizes["pipe"]
    padded = -(-rows // LANES) * LANES
    others = max(chips - 1, 1)
    rounds = max(sizes["pipe"] - 2, 0) + sizes["tensor"]
    f32 = jnp.float32
    dma = pltpu.SemaphoreType.DMA
    vmem = pl.BlockSpec(memory_space=pltpu.VMEM)
    smem = pl.BlockSpec(memory_space=pltpu.SMEM)
    hbm = pl.BlockSpec(memory_space=pltpu.HBM)
    state = jax.ShapeDtypeStruct(master.shape, f32)
    block = rows * columns * 4
    inputs = (owner_order, drop_flags.reshape(drop_flags.shape[-3:]), grad_parts, master, moment_m, moment_v)
    total, held, stats = pl.pallas_call(
        functools.partial(exchange, sizes, stages, cuts),
        out_shape=tuple(pltpu.VMEM(shape, f32) for shape in ((rows, width), (3, rows, width), (3 * SUBLANES, LANES))),
        in_specs=[smem] + [hbm] * 6,
        out_specs=(vmem,) * 3,
        scratch_shapes=[
            pltpu.SMEM((n,), jnp.int32),
            pltpu.VMEM((1, 1, rows), jnp.int32),
            [pltpu.VMEM((n, end - start, width), f32) for start, end in zip(cuts, cuts[1:])],
            pltpu.VMEM((chips, rows, width), f32),
            pltpu.VMEM((chips, rows, width), f32),
            pltpu.VMEM((others, rows, width), f32),
            pltpu.VMEM((others, rows, width), f32),
            pltpu.VMEM((1, 1, padded), f32),
            pltpu.VMEM((n - 1, 1, padded), f32),
            [pltpu.VMEM((2, LANES), f32) for _ in peers],
            [pltpu.VMEM((max(size, 1), 2, LANES), f32) for size in peers],
            pltpu.VMEM((PIECES - 1, 16, width // PIECES), f32),
            dma((2,)),
            dma((len(cuts) - 1,)),
            dma((1,)),
            dma((1,)),
            dma((len(cuts),)),
            dma((1,)),
            dma((len(cuts) - 1, others)),
            dma((2,)),
            dma((len(peers), 2)),
            dma((PIECES - 1,)),
            pltpu.SemaphoreType.REGULAR((3,)),
            pltpu.SemaphoreType.REGULAR((rounds,)),
        ],
        compiler_params=pltpu.CompilerParams(
            collective_id=0, has_side_effects=True, vmem_limit_bytes=8 * block
        ),
        cost_estimate=pl.CostEstimate(
            flops=8 * rows * columns, bytes_accessed=20 * rows * columns * 4, transcendentals=0
        ),
    )(step_count, *(pltpu.with_memory_space_constraint(x, pltpu.HBM) for x in inputs))
    outs = pl.pallas_call(
        functools.partial(update, entries, chunks),
        out_shape=(state, state, state, state, jax.ShapeDtypeStruct((1,), jnp.int32)),
        in_specs=[vmem] * 3,
        out_specs=(hbm,) * 5,
        scratch_shapes=[pltpu.VMEM((4, rows, width), f32), pltpu.SMEM((1,), jnp.int32), dma((5,))],
        compiler_params=pltpu.CompilerParams(vmem_limit_bytes=8 * block),
        cost_estimate=pl.CostEstimate(
            flops=20 * rows * width, bytes_accessed=8 * rows * width * 4, transcendentals=0
        ),
    )(stats, total, held)
    return (*outs[:4], outs[4].reshape(()))


def solution(mesh):
    return jax.shard_map(
        functools.partial(body, dict(mesh.shape)),
        mesh=mesh,
        in_specs=(
            P("dp", "pipe", "tensor", None, None),
            P("dp", "pipe", "tensor", None),
            P(),
            P(),
            P("pipe", "tensor", None, "dp"),
            P("pipe", "tensor", None, "dp"),
            P("pipe", "tensor", None, "dp"),
        ),
        out_specs=(
            P("pipe", "tensor", None, "dp"),
            P("pipe", "tensor", None, "dp"),
            P("pipe", "tensor", None, "dp"),
            P("pipe", "tensor", None, "dp"),
            P(),
        ),
        check_vma=False,
    )
```

```python
import functools
import itertools
import math
import jax
import jax.numpy as jnp
from jax import lax
from jax.experimental import pallas as pl
from jax.experimental.pallas import tpu as pltpu
from jax.sharding import PartitionSpec as P

AXES = ("dp", "tensor", "pipe")
MESH = pl.DeviceIdType.MESH
LANES = 128
SUBLANES = 8
DIRECT = 64
EDGES = (0, 3, 8, 11, 16)
PIECES = len(EDGES) - 1


def as_column(row, rows):
    square = (rows, rows)
    diagonal = lax.broadcasted_iota(jnp.int32, square, 0) == lax.broadcasted_iota(jnp.int32, square, 1)
    return jnp.sum(jnp.where(diagonal, jnp.broadcast_to(row, square), 0.0), axis=1, keepdims=True)


def int_power(base, exponent):
    result = jnp.ones(exponent.shape, jnp.float32)
    square = jnp.full(exponent.shape, base, jnp.float32)
    for bit in range(31):
        result = jnp.where((exponent >> bit) & 1 == 1, result * square, result)
        square = square * square
    return result


def can_relay(sizes, stages):
    return sizes["dp"] == 4 and sizes["tensor"] == 2 and len(stages) == 1 and sizes["pipe"] > 1


def exchange(
    sizes, stages, cuts,
    step_ref, order_hbm, flags_hbm, grad_hbm, w_hbm, m_hbm, v_hbm,
    total, held, stats,
    order_ref, flags_ref, g_bufs, pair_send, pair_recv, ring_send, ring_recv,
    kept_send, kept_recv, red_sends, red_recvs,
    relay_buf, tail_send, tail_recv, tail_ring, o_sem, g_sem, w_sem, ps_sem, pr_sem, rs_sem, rr_sem, k_sem, a_sem, via_sem, tail_sem, chain_sem, ready_sem,
):
    n = sizes["dp"]
    chips = n // 2
    relayed = can_relay(sizes, stages)
    rows, width = total.shape
    parts = [(start, end - start) for start, end in zip(cuts, cuts[1:])]
    me = {axis: lax.axis_index(axis) for axis in AXES}
    chip, core = lax.div(me["dp"], 2), lax.rem(me["dp"], 2)

    def peer(offsets):
        return {axis: lax.rem(me[axis] + off, sizes[axis]) for axis, off in offsets.items()}

    def offsets_of(axes):
        ranges = [range(sizes[axis]) for axis in axes]
        return [dict(zip(axes, offs)) for offs in itertools.product(*ranges) if any(offs)]

    small = [
        pltpu.make_async_copy(flags_hbm, flags_ref, o_sem.at[0]),
        pltpu.make_async_copy(order_hbm, order_ref, o_sem.at[1]),
    ]
    for copy in small:
        copy.start()
    loads = []

    def load(k):
        start, size = parts[k]
        for b in range(n):
            pltpu.make_async_copy(
                grad_hbm.at[0, 0, 0, pl.ds(start, size), pl.ds(b * width, width)], g_bufs[k].at[b], g_sem.at[k]
            ).start()
        loads.append(pltpu.make_async_copy(g_bufs[k], g_bufs[k], g_sem.at[k]))

    load(0)

    def greet(sem, axis):
        if axis == "dp":
            for off in range(1, n):
                pl.semaphore_signal(sem, inc=1, device_id=peer({"dp": off}), device_id_type=MESH)
            return n - 1
        at, last = me[axis], sizes[axis] - 1

        @pl.when(at > 0)
        def _():
            pl.semaphore_signal(sem, inc=1, device_id={**home, axis: at - 1}, device_id_type=MESH)

        @pl.when(at < last)
        def _():
            pl.semaphore_signal(sem, inc=1, device_id={**home, axis: at + 1}, device_id_type=MESH)

        return jnp.minimum(at, 1) + jnp.minimum(last - at, 1)

    sibling = {"dp": chip * 2 + 1 - core}
    barrier = pltpu.get_barrier_semaphore()

    @pl.when(core == 1)
    def _():
        pl.semaphore_signal(barrier, inc=1, device_id=sibling, device_id_type=MESH)

    home = {"dp": chip * 2 + 1}
    for off in range(1, chips):
        pl.semaphore_signal(
            barrier, inc=1, device_id={"dp": lax.rem(chip + off, chips) * 2 + 1}, device_id_type=MESH
        )
    met = 2 * (chips - 1 + greet(barrier, "tensor") + greet(barrier, "pipe"))
    home = {}
    rounds = ["pipe"] * max(sizes["pipe"] - 2, 0) + ["tensor"] * (sizes["tensor"] - 1) + ["dp"]
    left, owed = list(rounds), []

    def next_round():
        if owed:
            at, amount = owed.pop()
            pl.semaphore_wait(ready_sem.at[at], amount)
        if left:
            at = len(rounds) - len(left)
            owed.append((at, greet(ready_sem.at[at], left.pop(0))))

    load(1)

    @pl.when(core == 0)
    def _():
        pl.semaphore_wait(barrier, 1)
        pl.semaphore_signal(chain_sem.at[2], inc=1, device_id=sibling, device_id_type=MESH)

    for copy in small:
        copy.wait()
    for k in range(2, len(parts)):
        load(k)
    flags_row = flags_ref[0].astype(jnp.float32)
    kept_row = 1.0 - flags_row
    kept = as_column(kept_row, rows)
    kept_send[0, :, 0:rows] = kept_row
    dropped = jnp.sum(flags_row, axis=1, keepdims=True)

    def chip_at(slot):
        return lax.rem(chip + slot, chips)

    def term(k, owner):
        start, size = parts[k]
        return g_bufs[k][order_ref[owner]] * kept[start:start + size]

    def rows_of(ref, slot, k):
        start, size = parts[k]
        return ref.at[slot, pl.ds(start, size)]

    pair = {}

    def send_pair(k, slot):
        copy = pltpu.make_async_remote_copy(
            rows_of(pair_send, slot, k), rows_of(pair_recv, slot, k),
            ps_sem.at[1 if slot else 0], pr_sem.at[k if slot else len(parts)],
            device_id=sibling, device_id_type=MESH,
        )
        copy.start()
        pair[k, slot] = copy

    far = list(range(1, chips))
    def to_sibling(k):
        start, size = parts[k]
        with jax.named_scope(f"load_wait{k}"):
            loads[k].wait()
        for slot in far:
            pair_send[slot, start:start + size, :] = term(k, chip_at(slot) * 2 + 1 - core)
        if k == 0:
            with jax.named_scope("sibling_wait"):
                @pl.when(core == 1)
                def _():
                    pl.semaphore_wait(chain_sem.at[2], 1)
        for slot in far:
            send_pair(k, slot)

    kepts = pltpu.make_async_remote_copy(
        kept_recv, kept_recv, k_sem.at[0], k_sem.at[1], device_id=sibling, device_id_type=MESH
    )

    ring = {}
    swing = len(parts) - 2
    far_end = sizes["pipe"] - 1
    gap = 2 * me["pipe"] - far_end
    across = {"dp": chip_at(1) * 2 + core}
    lend = [gap >= 1, gap >= 3, 2 * me["tensor"] >= sizes["tensor"]] if relayed else []
    borrow = [gap <= -1, gap <= -3, 2 * me["tensor"] < sizes["tensor"]] if relayed else []
    mirror = [{"pipe": far_end - me["pipe"]}] * 2 + [{"tensor": sizes["tensor"] - 1 - me["tensor"]}]
    edges = [width * edge // 16 for edge in EDGES]

    def piece(ref, h):
        start, size = parts[swing]
        return ref.at[0, pl.ds(start, size), pl.ds(edges[h], edges[h + 1] - edges[h])]

    def lodging(h):
        return relay_buf.at[h, :, pl.ds(0, edges[h + 1] - edges[h])]

    def swing_copy(h):
        return pltpu.make_async_remote_copy(
            piece(ring_send, h), piece(ring_recv, h), rs_sem.at[0], rr_sem.at[swing, 0],
            device_id=across, device_id_type=MESH,
        )

    def via_copy(h):
        return pltpu.make_async_remote_copy(
            piece(ring_send, h), lodging(h), rs_sem.at[0], via_sem.at[h],
            device_id={**across, **mirror[h]}, device_id_type=MESH,
        )

    def forward_copy(h):
        return pltpu.make_async_remote_copy(
            lodging(h), piece(ring_recv, h), via_sem.at[h], rr_sem.at[swing, 0],
            device_id=mirror[h], device_id_type=MESH,
        )

    def climb():
        at = me["pipe"]

        @pl.when(at >= 2)
        def _():
            pl.semaphore_wait(chain_sem.at[0], 1)

        @pl.when((at >= 1) & (at < far_end))
        def _():
            pl.semaphore_signal(chain_sem.at[0], inc=1, device_id={"pipe": at + 1}, device_id_type=MESH)

        @pl.when(lend[0] | lend[2])
        def _():
            pl.semaphore_signal(chain_sem.at[1], inc=1, device_id=across, device_id_type=MESH)

    tail = len(parts) - 1
    tail_at = pl.ds(*parts[tail])
    abroad = chip_at(1) * 2

    def tail_pair():
        return pltpu.make_async_remote_copy(
            tail_send, tail_recv, tail_sem.at[0], tail_sem.at[0], device_id=sibling, device_id_type=MESH
        )

    def tail_copy(c):
        return pltpu.make_async_remote_copy(
            tail_ring.at[c], ring_recv.at[0, tail_at], tail_sem.at[1], rr_sem.at[tail, 0],
            device_id={"dp": abroad + c}, device_id_type=MESH,
        )

    def tail_to_sibling():
        loads[tail].wait()

        @pl.when(core == 0)
        def _():
            for c in range(2):
                tail_send[c] = term(tail, abroad + c)
            tail_pair().start()

    def tail_to_owner():
        @pl.when(core == 1)
        def _():
            tail_pair().wait_recv()
            for c in range(2):
                tail_ring[c] = tail_recv[c] + term(tail, abroad + c)
                tail_copy(c).start()

    def to_owner(k):
        start, size = parts[k]
        for slot in far:
            target = chip_at(slot) * 2 + core
            mine = term(k, target)
            with jax.named_scope(f"pair_wait{k}"):
                if slot == far[0]:
                    pltpu.make_async_remote_copy(
                        pair_recv.at[pl.ds(1, chips - 1), pl.ds(start, size)],
                        pair_recv.at[pl.ds(1, chips - 1), pl.ds(start, size)],
                        ps_sem.at[0], pr_sem.at[k], device_id=sibling, device_id_type=MESH,
                    ).wait_recv()
            ring_send[slot - 1, start:start + size, :] = pair_recv[slot, start:start + size, :] + mine
            if relayed and k == swing:
                @pl.when(lend[0] | lend[2])
                def _():
                    with jax.named_scope("chain_wait"):
                        pl.semaphore_wait(chain_sem.at[1], 1)

                for h, away in enumerate(lend):
                    @pl.when(away)
                    def _():
                        via_copy(h).start()

                for h, away in enumerate(lend):
                    @pl.when(jnp.logical_not(away))
                    def _():
                        swing_copy(h).start()
                for h in range(len(lend), PIECES):
                    swing_copy(h).start()
                continue
            copy = pltpu.make_async_remote_copy(
                rows_of(ring_send, slot - 1, k), rows_of(ring_recv, slot - 1, k),
                rs_sem.at[0], rr_sem.at[k, slot - 1],
                device_id={"dp": target}, device_id_type=MESH,
            )
            copy.start()
            ring[k, slot] = copy

    to_sibling(0)
    to_sibling(1)
    with jax.named_scope("barrier_wait"):
        @pl.when(core == 1)
        def _():
            pl.semaphore_wait(barrier, met)
            pl.semaphore_signal(chain_sem.at[2], inc=1, device_id=sibling, device_id_type=MESH)

        @pl.when(core == 0)
        def _():
            pl.semaphore_wait(chain_sem.at[2], 1)
    for off in range(1, n):
        pltpu.make_async_remote_copy(
            kept_send.at[0], kept_recv.at[off - 1], k_sem.at[0], k_sem.at[1],
            device_id=peer({"dp": off}), device_id_type=MESH,
        ).start()
    to_owner(0)
    if relayed:
        climb()
    else:
        to_owner(1)
    if relayed:
        tail_to_sibling()
        to_sibling(swing)
        to_owner(1)
        tail_to_owner()
        to_owner(swing)
    else:
        for k in range(2, len(parts)):
            to_sibling(k)
        for k in range(2, len(parts)):
            to_owner(k)

    next_round()
    for k, (start, size) in enumerate(parts):
        pair_send[0, start:start + size, :] = term(k, chip * 2 + 1 - core)
        send_pair(k, 0)
    with jax.named_scope("kept_wait"):
        kepts.wait_recv()
    count_row = kept_row
    for i in range(n - 1):
        count_row = count_row + kept_recv[i, :, 0:rows]
    inverse = 1.0 / jnp.maximum(as_column(count_row, rows), 1.0)
    for i, source in enumerate((w_hbm, m_hbm, v_hbm)):
        pltpu.make_async_copy(source.at[0, 0], held.at[i], w_sem.at[0]).start()

    pltpu.make_async_remote_copy(
        pair_recv.at[0], pair_recv.at[0], ps_sem.at[0], pr_sem.at[len(parts)],
        device_id=sibling, device_id_type=MESH,
    ).wait_recv()
    for k, (start, size) in enumerate(parts):
        total[start:start + size, :] = pair_recv[0, start:start + size, :] + term(k, me["dp"])
    pltpu.make_async_copy(held, held, w_sem.at[0]).wait()
    held[1] = 0.9 * held[1]
    held[2] = 0.999 * held[2]
    steps = jnp.full((SUBLANES, LANES), step_ref[...], jnp.int32)
    stats[0:8, :] = jnp.zeros((SUBLANES, LANES), jnp.float32)
    stats[8:16, :] = 1.0 / (1.0 - int_power(0.9, steps))
    stats[16:24, :] = 1.0 / (1.0 - int_power(0.999, steps))

    if relayed:
        for h in (2, 0, 1):
            @pl.when(borrow[h])
            def _():
                with jax.named_scope(f"relay_wait{h}"):
                    via_copy(h).wait_recv()
                forward_copy(h).start()

    per_part = -(-(len(rounds) + 1) // max(len(parts) - 1, 1))
    squares = jnp.zeros((SUBLANES, LANES), jnp.float32)
    for k, (start, size) in enumerate(parts):
        at = slice(start, start + size)
        value = total[at, :]
        for slot in far:
            with jax.named_scope(f"ring_wait{k}"):
                if relayed and k == swing:
                    pltpu.make_async_remote_copy(
                        ring_recv.at[0, pl.ds(start, size)], ring_recv.at[0, pl.ds(start, size)],
                        rs_sem.at[0], rr_sem.at[swing, 0], device_id=across, device_id_type=MESH,
                    ).wait_recv()
                elif relayed and k == tail:
                    tail_copy(0).wait_recv()
                else:
                    ring[k, slot].wait_recv()
            value = value + ring_recv[slot - 1, at, :]
        value = value * inverse[at]
        total[at, :] = value
        squares = squares + jnp.sum(
            (value * value).reshape(size // SUBLANES, SUBLANES, width // LANES, LANES), axis=(0, 2)
        )
        for _ in range(per_part):
            next_round()

    result = [jnp.sum(squares, axis=0, keepdims=True), jnp.broadcast_to(dropped, (1, LANES))]
    done = []
    for stage, (axes, send, recv) in enumerate(zip(stages, red_sends, red_recvs)):
        for i, row in enumerate(result):
            send[i:i + 1, :] = row
        with jax.named_scope("norm_send"):
            back, stride = 0, 1
            for axis in reversed(axes):
                back, stride = back + lax.rem(sizes[axis] - me[axis], sizes[axis]) * stride, stride * sizes[axis]

            def share(i, device):
                pltpu.make_async_remote_copy(
                    send, recv.at[i], a_sem.at[stage, 0], a_sem.at[stage, 1],
                    device_id=device, device_id_type=MESH,
                ).start()

            @pl.when(back > 0)
            def _():
                share(back - 1, dict.fromkeys(axes, 0))

            for i, off in enumerate(offsets_of(axes)):
                @pl.when(back != i + 1)
                def _():
                    share(i, peer(off))
        copy = pltpu.make_async_remote_copy(
            recv, recv, a_sem.at[stage, 0], a_sem.at[stage, 1], device_id=sibling, device_id_type=MESH
        )
        done.append(copy)
        with jax.named_scope("norm_wait"):
            copy.wait_recv()
        for i in range(len(offsets_of(axes))):
            result = [row + recv[i, j:j + 1, :] for j, row in enumerate(result)]
    for i, row in enumerate(result):
        stats[i:i + 1, :] = row

    with jax.named_scope("send_wait"):
        sent = pl.ds(0, parts[tail][0] if relayed else rows)
        slots = pl.ds(0, chips - 1)
        pltpu.make_async_remote_copy(
            pair_send.at[0], pair_recv.at[0], ps_sem.at[0], pr_sem.at[0], device_id=sibling, device_id_type=MESH
        ).wait_send()
        kepts.wait_send()
        if far:
            pltpu.make_async_remote_copy(
                ring_send.at[slots, sent], ring_recv.at[slots, sent], ps_sem.at[1], pr_sem.at[0],
                device_id=sibling, device_id_type=MESH,
            ).wait_send()
            pltpu.make_async_remote_copy(
                ring_send.at[slots, sent], ring_recv.at[slots, sent], rs_sem.at[0], rr_sem.at[0, 0],
                device_id=sibling, device_id_type=MESH,
            ).wait_send()
        for copy in done:
            copy.wait_send()
        if relayed:
            @pl.when(core == 0)
            def _():
                tail_pair().wait_send()

            @pl.when(core == 1)
            def _():
                pltpu.make_async_remote_copy(
                    tail_ring, tail_recv, tail_sem.at[1], tail_sem.at[0], device_id=sibling, device_id_type=MESH
                ).wait_send()

            for h, taken in enumerate(borrow):
                @pl.when(taken)
                def _():
                    forward_copy(h).wait_send()


def update(
    entries, chunks, stats, grad_ref, held,
    w_out, m_out, v_out, dir_out, drop_out, bufs, drop_ref, sems,
):
    rows, width = grad_ref.shape
    part = rows // chunks
    scale_m = jnp.concatenate([stats[8:16, :]] * (width // LANES), axis=1)
    scale_v = jnp.concatenate([stats[16:24, :]] * (width // LANES), axis=1)
    summed = jnp.sum(jnp.broadcast_to(stats[0:1, :], (SUBLANES, LANES)), axis=1, keepdims=True)
    rms = jnp.sqrt(summed * (1.0 / entries))
    clip = jnp.minimum(1.0, 0.05 / (rms + 1e-06))
    share_m, share_v = 0.1 * clip, math.sqrt(0.001) * clip
    outs = (w_out, m_out, v_out, dir_out)
    for k in range(chunks):
        at = slice(k * part, (k + 1) * part)
        grad = grad_ref[at, :]
        root = grad * share_v
        new_m = held[1, at, :] + grad * share_m
        new_v = held[2, at, :] + root * root
        weights = held[0, at, :]
        corrected = new_v * scale_v
        direction = (new_m * scale_m) / (corrected * lax.rsqrt(corrected) + 1e-08) + 0.1 * weights
        values = (weights - 0.001 * direction, new_m, new_v, direction)
        for i, (value, out) in enumerate(zip(values, outs)):
            bufs[i, at, :] = value
            pltpu.make_async_copy(bufs.at[i, pl.ds(k * part, part)], out.at[0, 0, pl.ds(k * part, part)], sems.at[i]).start()
        if k == 0:
            drop_ref[0] = jnp.max(stats[1:2, :]).astype(jnp.int32)
            drop = pltpu.make_async_copy(drop_ref, drop_out, sems.at[4])
            drop.start()
    for i, out in enumerate(outs):
        pltpu.make_async_copy(bufs.at[i], out.at[0, 0], sems.at[i]).wait()
    drop.wait()


def body(sizes, grad_parts, drop_flags, owner_order, step_count, master, moment_m, moment_v):
    n = sizes["dp"]
    chips = n // 2
    rows, columns = grad_parts.shape[-2:]
    width = master.shape[-1]
    chunks = rows // 8
    cuts = sorted({0, 8, rows - 24, rows - 8, rows})
    devices = n * sizes["tensor"] * sizes["pipe"]
    stages = [AXES] if devices <= DIRECT else [(axis,) for axis in AXES]
    peers = []
    for axes in stages:
        size = 1
        for axis in axes:
            size *= sizes[axis]
        peers.append(size - 1)
    entries = rows * columns * sizes["tensor"] * sizes["pipe"]
    padded = -(-rows // LANES) * LANES
    others = max(chips - 1, 1)
    rounds = max(sizes["pipe"] - 2, 0) + sizes["tensor"]
    f32 = jnp.float32
    dma = pltpu.SemaphoreType.DMA
    vmem = pl.BlockSpec(memory_space=pltpu.VMEM)
    smem = pl.BlockSpec(memory_space=pltpu.SMEM)
    hbm = pl.BlockSpec(memory_space=pltpu.HBM)
    state = jax.ShapeDtypeStruct(master.shape, f32)
    block = rows * columns * 4
    inputs = (owner_order, drop_flags.reshape(drop_flags.shape[-3:]), grad_parts, master, moment_m, moment_v)
    total, held, stats = pl.pallas_call(
        functools.partial(exchange, sizes, stages, cuts),
        out_shape=tuple(pltpu.VMEM(shape, f32) for shape in ((rows, width), (3, rows, width), (3 * SUBLANES, LANES))),
        in_specs=[smem] + [hbm] * 6,
        out_specs=(vmem,) * 3,
        scratch_shapes=[
            pltpu.SMEM((n,), jnp.int32),
            pltpu.VMEM((1, 1, rows), jnp.int32),
            [pltpu.VMEM((n, end - start, width), f32) for start, end in zip(cuts, cuts[1:])],
            pltpu.VMEM((chips, rows, width), f32),
            pltpu.VMEM((chips, rows, width), f32),
            pltpu.VMEM((others, rows, width), f32),
            pltpu.VMEM((others, rows, width), f32),
            pltpu.VMEM((1, 1, padded), f32),
            pltpu.VMEM((n - 1, 1, padded), f32),
            [pltpu.VMEM((2, LANES), f32) for _ in peers],
            [pltpu.VMEM((max(size, 1), 2, LANES), f32) for size in peers],
            pltpu.VMEM((PIECES - 1, 16, width // 2), f32),
            pltpu.VMEM((2, 8, width), f32),
            pltpu.VMEM((2, 8, width), f32),
            pltpu.VMEM((2, 8, width), f32),
            dma((2,)),
            dma((len(cuts) - 1,)),
            dma((1,)),
            dma((2,)),
            dma((len(cuts),)),
            dma((1,)),
            dma((len(cuts) - 1, others)),
            dma((2,)),
            dma((len(peers), 2)),
            dma((PIECES - 1,)),
            dma((2,)),
            pltpu.SemaphoreType.REGULAR((3,)),
            pltpu.SemaphoreType.REGULAR((rounds,)),
        ],
        compiler_params=pltpu.CompilerParams(
            collective_id=0, has_side_effects=True, vmem_limit_bytes=8 * block
        ),
        cost_estimate=pl.CostEstimate(
            flops=8 * rows * columns, bytes_accessed=20 * rows * columns * 4, transcendentals=0
        ),
    )(step_count, *(pltpu.with_memory_space_constraint(x, pltpu.HBM) for x in inputs))
    outs = pl.pallas_call(
        functools.partial(update, entries, chunks),
        out_shape=(state, state, state, state, jax.ShapeDtypeStruct((1,), jnp.int32)),
        in_specs=[vmem] * 3,
        out_specs=(hbm,) * 5,
        scratch_shapes=[pltpu.VMEM((4, rows, width), f32), pltpu.SMEM((1,), jnp.int32), dma((5,))],
        compiler_params=pltpu.CompilerParams(vmem_limit_bytes=8 * block),
        cost_estimate=pl.CostEstimate(
            flops=20 * rows * width, bytes_accessed=8 * rows * width * 4, transcendentals=0
        ),
    )(stats, total, held)
    return (*outs[:4], outs[4].reshape(()))


def solution(mesh):
    return jax.shard_map(
        functools.partial(body, dict(mesh.shape)),
        mesh=mesh,
        in_specs=(
            P("dp", "pipe", "tensor", None, None),
            P("dp", "pipe", "tensor", None),
            P(),
            P(),
            P("pipe", "tensor", None, "dp"),
            P("pipe", "tensor", None, "dp"),
            P("pipe", "tensor", None, "dp"),
        ),
        out_specs=(
            P("pipe", "tensor", None, "dp"),
            P("pipe", "tensor", None, "dp"),
            P("pipe", "tensor", None, "dp"),
            P("pipe", "tensor", None, "dp"),
            P(),
        ),
        check_vma=False,
    )
```

```python
import functools
import itertools
import math
import jax
import jax.numpy as jnp
from jax import lax
from jax.experimental import pallas as pl
from jax.experimental.pallas import tpu as pltpu
from jax.sharding import PartitionSpec as P

AXES = ("dp", "tensor", "pipe")
MESH = pl.DeviceIdType.MESH
LANES = 128
SUBLANES = 8
DIRECT = 64
EDGES = (0, 3, 8, 11, 16)
PIECES = len(EDGES) - 1


def as_column(row, rows):
    square = (rows, rows)
    diagonal = lax.broadcasted_iota(jnp.int32, square, 0) == lax.broadcasted_iota(jnp.int32, square, 1)
    return jnp.sum(jnp.where(diagonal, jnp.broadcast_to(row, square), 0.0), axis=1, keepdims=True)


def int_power(base, exponent):
    result = jnp.ones(exponent.shape, jnp.float32)
    square = jnp.full(exponent.shape, base, jnp.float32)
    for bit in range(31):
        result = jnp.where((exponent >> bit) & 1 == 1, result * square, result)
        square = square * square
    return result


def can_relay(sizes, stages):
    return sizes["dp"] == 4 and sizes["tensor"] == 2 and len(stages) == 1 and sizes["pipe"] > 1


def exchange(
    sizes, stages, cuts,
    step_ref, order_hbm, flags_hbm, grad_hbm, w_hbm, m_hbm, v_hbm,
    total, held, stats,
    order_ref, flags_ref, g_bufs, pair_send, pair_recv, ring_send, ring_recv,
    kept_send, kept_recv, red_sends, red_recvs,
    step_send, step_recv, relay_buf, tail_send, tail_recv, tail_ring, o_sem, g_sem, w_sem, ps_sem, pr_sem, rs_sem, rr_sem, k_sem, a_sem, via_sem, step_sem, tail_sem, chain_sem, ready_sem,
):
    n = sizes["dp"]
    chips = n // 2
    relayed = can_relay(sizes, stages)
    rows, width = total.shape
    parts = [(start, end - start) for start, end in zip(cuts, cuts[1:])]
    me = {axis: lax.axis_index(axis) for axis in AXES}
    chip, core = lax.div(me["dp"], 2), lax.rem(me["dp"], 2)

    def peer(offsets):
        return {axis: lax.rem(me[axis] + off, sizes[axis]) for axis, off in offsets.items()}

    def offsets_of(axes):
        ranges = [range(sizes[axis]) for axis in axes]
        return [dict(zip(axes, offs)) for offs in itertools.product(*ranges) if any(offs)]

    small = [
        pltpu.make_async_copy(flags_hbm, flags_ref, o_sem.at[0]),
        pltpu.make_async_copy(order_hbm, order_ref, o_sem.at[1]),
    ]
    for copy in small:
        copy.start()
    loads = []

    def load(k):
        start, size = parts[k]
        for b in range(n):
            pltpu.make_async_copy(
                grad_hbm.at[0, 0, 0, pl.ds(start, size), pl.ds(b * width, width)], g_bufs[k].at[b], g_sem.at[k]
            ).start()
        loads.append(pltpu.make_async_copy(g_bufs[k], g_bufs[k], g_sem.at[k]))

    load(0)

    def greet(sem, axis):
        if axis == "dp":
            for off in range(1, n):
                pl.semaphore_signal(sem, inc=1, device_id=peer({"dp": off}), device_id_type=MESH)
            return n - 1
        at, last = me[axis], sizes[axis] - 1

        @pl.when(at > 0)
        def _():
            pl.semaphore_signal(sem, inc=1, device_id={**home, axis: at - 1}, device_id_type=MESH)

        @pl.when(at < last)
        def _():
            pl.semaphore_signal(sem, inc=1, device_id={**home, axis: at + 1}, device_id_type=MESH)

        return jnp.minimum(at, 1) + jnp.minimum(last - at, 1)

    sibling = {"dp": chip * 2 + 1 - core}
    barrier = pltpu.get_barrier_semaphore()

    @pl.when(core == 1)
    def _():
        pl.semaphore_signal(barrier, inc=1, device_id=sibling, device_id_type=MESH)

    home = {"dp": chip * 2 + 1}
    for off in range(1, chips):
        pl.semaphore_signal(
            barrier, inc=1, device_id={"dp": lax.rem(chip + off, chips) * 2 + 1}, device_id_type=MESH
        )
    met = 2 * (chips - 1 + greet(barrier, "tensor") + greet(barrier, "pipe"))
    home = {}
    rounds = ["pipe"] * max(sizes["pipe"] - 2, 0) + ["tensor"] * (sizes["tensor"] - 1) + ["dp"]
    left, owed = list(rounds), []

    def next_round():
        if owed:
            at, amount = owed.pop()
            pl.semaphore_wait(ready_sem.at[at], amount)
        if left:
            at = len(rounds) - len(left)
            owed.append((at, greet(ready_sem.at[at], left.pop(0))))

    load(1)

    @pl.when(core == 0)
    def _():
        pl.semaphore_wait(barrier, 1)
        pl.semaphore_signal(chain_sem.at[2], inc=1, device_id=sibling, device_id_type=MESH)

    for copy in small:
        copy.wait()
    for k in range(2, len(parts)):
        load(k)
    flags_row = flags_ref[0].astype(jnp.float32)
    kept_row = 1.0 - flags_row
    kept = as_column(kept_row, rows)
    kept_send[0, :, 0:rows] = kept_row
    dropped = jnp.sum(flags_row, axis=1, keepdims=True)

    def chip_at(slot):
        return lax.rem(chip + slot, chips)

    def term(k, owner):
        start, size = parts[k]
        return g_bufs[k][order_ref[owner]] * kept[start:start + size]

    def rows_of(ref, slot, k):
        start, size = parts[k]
        return ref.at[slot, pl.ds(start, size)]

    pair = {}

    def send_pair(k, slot):
        copy = pltpu.make_async_remote_copy(
            rows_of(pair_send, slot, k), rows_of(pair_recv, slot, k),
            ps_sem.at[1 if slot else 0], pr_sem.at[k if slot else len(parts)],
            device_id=sibling, device_id_type=MESH,
        )
        copy.start()
        pair[k, slot] = copy

    far = list(range(1, chips))
    def to_sibling(k):
        start, size = parts[k]
        with jax.named_scope(f"load_wait{k}"):
            loads[k].wait()
        for slot in far:
            pair_send[slot, start:start + size, :] = term(k, chip_at(slot) * 2 + 1 - core)
        if k == 0:
            with jax.named_scope("sibling_wait"):
                @pl.when(core == 1)
                def _():
                    pl.semaphore_wait(chain_sem.at[2], 1)
        for slot in far:
            send_pair(k, slot)

    kepts = pltpu.make_async_remote_copy(
        kept_recv, kept_recv, k_sem.at[0], k_sem.at[1], device_id=sibling, device_id_type=MESH
    )

    ring = {}
    swing = len(parts) - 2
    far_end = sizes["pipe"] - 1
    gap = 2 * me["pipe"] - far_end
    across = {"dp": chip_at(1) * 2 + core}
    lend = [gap >= 1, gap >= 3, 2 * me["tensor"] >= sizes["tensor"]] if relayed else []
    borrow = [gap <= -1, gap <= -3, 2 * me["tensor"] < sizes["tensor"]] if relayed else []
    mirror = [{"pipe": far_end - me["pipe"]}] * 2 + [{"tensor": sizes["tensor"] - 1 - me["tensor"]}]
    edges = [width * edge // 16 for edge in EDGES]

    def piece(ref, h):
        start, size = parts[swing]
        return ref.at[0, pl.ds(start, size), pl.ds(edges[h], edges[h + 1] - edges[h])]

    def lodging(h):
        return relay_buf.at[h, :, pl.ds(0, edges[h + 1] - edges[h])]

    def swing_copy(h):
        return pltpu.make_async_remote_copy(
            piece(ring_send, h), piece(ring_recv, h), rs_sem.at[0], rr_sem.at[swing, 0],
            device_id=across, device_id_type=MESH,
        )

    def via_copy(h):
        return pltpu.make_async_remote_copy(
            piece(ring_send, h), lodging(h), rs_sem.at[0], via_sem.at[h],
            device_id={**across, **mirror[h]}, device_id_type=MESH,
        )

    def forward_copy(h):
        return pltpu.make_async_remote_copy(
            lodging(h), piece(ring_recv, h), via_sem.at[h], rr_sem.at[swing, 0],
            device_id=mirror[h], device_id_type=MESH,
        )

    def climb():
        at = me["pipe"]

        @pl.when(at >= 2)
        def _():
            pl.semaphore_wait(chain_sem.at[0], 1)

        @pl.when((at >= 1) & (at < far_end))
        def _():
            pl.semaphore_signal(chain_sem.at[0], inc=1, device_id={"pipe": at + 1}, device_id_type=MESH)

        @pl.when(lend[0] | lend[2])
        def _():
            pl.semaphore_signal(chain_sem.at[1], inc=1, device_id=across, device_id_type=MESH)

    tail = len(parts) - 1
    tail_at = pl.ds(*parts[tail])
    abroad = chip_at(1) * 2

    def tail_pair():
        return pltpu.make_async_remote_copy(
            tail_send, tail_recv, tail_sem.at[0], tail_sem.at[0], device_id=sibling, device_id_type=MESH
        )

    def tail_copy(c):
        return pltpu.make_async_remote_copy(
            tail_ring.at[c], ring_recv.at[0, tail_at], tail_sem.at[1], rr_sem.at[tail, 0],
            device_id={"dp": abroad + c}, device_id_type=MESH,
        )

    def tail_to_sibling():
        loads[tail].wait()

        @pl.when(core == 0)
        def _():
            for c in range(2):
                tail_send[c] = term(tail, abroad + c)
            tail_pair().start()

    def tail_to_owner():
        @pl.when(core == 1)
        def _():
            tail_pair().wait_recv()
            for c in range(2):
                tail_ring[c] = tail_recv[c] + term(tail, abroad + c)
                tail_copy(c).start()

    def to_owner(k):
        start, size = parts[k]
        for slot in far:
            target = chip_at(slot) * 2 + core
            mine = term(k, target)
            with jax.named_scope(f"pair_wait{k}"):
                if slot == far[0]:
                    pltpu.make_async_remote_copy(
                        pair_recv.at[pl.ds(1, chips - 1), pl.ds(start, size)],
                        pair_recv.at[pl.ds(1, chips - 1), pl.ds(start, size)],
                        ps_sem.at[0], pr_sem.at[k], device_id=sibling, device_id_type=MESH,
                    ).wait_recv()
            ring_send[slot - 1, start:start + size, :] = pair_recv[slot, start:start + size, :] + mine
            if relayed and k == swing:
                @pl.when(lend[0] | lend[2])
                def _():
                    with jax.named_scope("chain_wait"):
                        pl.semaphore_wait(chain_sem.at[1], 1)

                for h, away in enumerate(lend):
                    @pl.when(away)
                    def _():
                        via_copy(h).start()

                for h, away in enumerate(lend):
                    @pl.when(jnp.logical_not(away))
                    def _():
                        swing_copy(h).start()
                for h in range(len(lend), PIECES):
                    swing_copy(h).start()
                continue
            copy = pltpu.make_async_remote_copy(
                rows_of(ring_send, slot - 1, k), rows_of(ring_recv, slot - 1, k),
                rs_sem.at[0], rr_sem.at[k, slot - 1],
                device_id={"dp": target}, device_id_type=MESH,
            )
            copy.start()
            ring[k, slot] = copy

    to_sibling(0)
    to_sibling(1)
    with jax.named_scope("barrier_wait"):
        @pl.when(core == 1)
        def _():
            pl.semaphore_wait(barrier, met)
            pl.semaphore_signal(chain_sem.at[2], inc=1, device_id=sibling, device_id_type=MESH)

        @pl.when(core == 0)
        def _():
            pl.semaphore_wait(chain_sem.at[2], 1)
    for off in range(1, n):
        pltpu.make_async_remote_copy(
            kept_send.at[0], kept_recv.at[off - 1], k_sem.at[0], k_sem.at[1],
            device_id=peer({"dp": off}), device_id_type=MESH,
        ).start()
    to_owner(0)
    if relayed:
        climb()
    else:
        to_owner(1)
    if relayed:
        tail_to_sibling()
        to_sibling(swing)
        to_owner(1)
        tail_to_owner()
        to_owner(swing)
    else:
        for k in range(2, len(parts)):
            to_sibling(k)
        for k in range(2, len(parts)):
            to_owner(k)

    next_round()
    for k, (start, size) in enumerate(parts):
        pair_send[0, start:start + size, :] = term(k, chip * 2 + 1 - core)
        send_pair(k, 0)
    with jax.named_scope("kept_wait"):
        kepts.wait_recv()
    count_row = kept_row
    for i in range(n - 1):
        count_row = count_row + kept_recv[i, :, 0:rows]
    inverse = 1.0 / jnp.maximum(as_column(count_row, rows), 1.0)
    next_round()
    for i, source in enumerate((w_hbm, m_hbm, v_hbm)):
        pltpu.make_async_copy(source.at[0, 0], held.at[i], w_sem.at[0]).start()

    pltpu.make_async_remote_copy(
        pair_recv.at[0], pair_recv.at[0], ps_sem.at[0], pr_sem.at[len(parts)],
        device_id=sibling, device_id_type=MESH,
    ).wait_recv()
    for k, (start, size) in enumerate(parts):
        total[start:start + size, :] = pair_recv[0, start:start + size, :] + term(k, me["dp"])
    pltpu.make_async_copy(held, held, w_sem.at[0]).wait()
    held[1] = 0.9 * held[1]
    held[2] = 0.999 * held[2]
    next_round()

    if relayed:
        for h in (2, 0, 1):
            @pl.when(borrow[h])
            def _():
                with jax.named_scope(f"relay_wait{h}"):
                    via_copy(h).wait_recv()
                forward_copy(h).start()

    while left or owed:
        next_round()
    first = functools.reduce(jnp.logical_and, [me[axis] == 0 for axis in stages[0]])

    def tell(device):
        return pltpu.make_async_remote_copy(
            step_send, step_recv, step_sem.at[0], step_sem.at[1], device_id=device, device_id_type=MESH
        )

    @pl.when(first)
    def _():
        step_send[...] = step_ref[...]
        step_recv[...] = step_ref[...]
        for off in offsets_of(stages[0]):
            tell(off).start()

    squares = jnp.zeros((SUBLANES, LANES), jnp.float32)
    for k, (start, size) in enumerate(parts):
        at = slice(start, start + size)
        value = total[at, :]
        for slot in far:
            with jax.named_scope(f"ring_wait{k}"):
                if relayed and k == swing:
                    pltpu.make_async_remote_copy(
                        ring_recv.at[0, pl.ds(start, size)], ring_recv.at[0, pl.ds(start, size)],
                        rs_sem.at[0], rr_sem.at[swing, 0], device_id=across, device_id_type=MESH,
                    ).wait_recv()
                elif relayed and k == tail:
                    tail_copy(0).wait_recv()
                else:
                    ring[k, slot].wait_recv()
            value = value + ring_recv[slot - 1, at, :]
        value = value * inverse[at]
        total[at, :] = value
        squares = squares + jnp.sum(
            (value * value).reshape(size // SUBLANES, SUBLANES, width // LANES, LANES), axis=(0, 2)
        )

    result = [jnp.sum(squares, axis=0, keepdims=True), jnp.broadcast_to(dropped, (1, LANES))]
    done = []
    for stage, (axes, send, recv) in enumerate(zip(stages, red_sends, red_recvs)):
        for i, row in enumerate(result):
            send[i:i + 1, :] = row
        with jax.named_scope("norm_send"):
            back, stride = 0, 1
            for axis in reversed(axes):
                back, stride = back + lax.rem(sizes[axis] - me[axis], sizes[axis]) * stride, stride * sizes[axis]

            def share(i, device):
                pltpu.make_async_remote_copy(
                    send, recv.at[i], a_sem.at[stage, 0], a_sem.at[stage, 1],
                    device_id=device, device_id_type=MESH,
                ).start()

            @pl.when(back > 0)
            def _():
                share(back - 1, dict.fromkeys(axes, 0))

            for i, off in enumerate(offsets_of(axes)):
                @pl.when(back != i + 1)
                def _():
                    share(i, peer(off))
        if stage == 0:
            @pl.when(jnp.logical_not(first))
            def _():
                tell(sibling).wait_recv()

            steps = jnp.broadcast_to(step_recv[0:1, :], (SUBLANES, LANES)).astype(jnp.int32)
            stats[0:8, :] = jnp.zeros((SUBLANES, LANES), jnp.float32)
            stats[8:16, :] = 1.0 / (1.0 - int_power(0.9, steps))
            stats[16:24, :] = 1.0 / (1.0 - int_power(0.999, steps))
        copy = pltpu.make_async_remote_copy(
            recv, recv, a_sem.at[stage, 0], a_sem.at[stage, 1], device_id=sibling, device_id_type=MESH
        )
        done.append(copy)
        with jax.named_scope("norm_wait"):
            copy.wait_recv()
        for i in range(len(offsets_of(axes))):
            result = [row + recv[i, j:j + 1, :] for j, row in enumerate(result)]
    for i, row in enumerate(result):
        stats[i:i + 1, :] = row

    with jax.named_scope("send_wait"):
        sent = pl.ds(0, parts[tail][0] if relayed else rows)
        slots = pl.ds(0, chips - 1)
        pltpu.make_async_remote_copy(
            pair_send.at[0], pair_recv.at[0], ps_sem.at[0], pr_sem.at[0], device_id=sibling, device_id_type=MESH
        ).wait_send()
        kepts.wait_send()
        if far:
            pltpu.make_async_remote_copy(
                ring_send.at[slots, sent], ring_recv.at[slots, sent], ps_sem.at[1], pr_sem.at[0],
                device_id=sibling, device_id_type=MESH,
            ).wait_send()
            pltpu.make_async_remote_copy(
                ring_send.at[slots, sent], ring_recv.at[slots, sent], rs_sem.at[0], rr_sem.at[0, 0],
                device_id=sibling, device_id_type=MESH,
            ).wait_send()
        for copy in done:
            copy.wait_send()

        @pl.when(first)
        def _():
            pltpu.make_async_remote_copy(
                red_recvs[0], red_recvs[0], step_sem.at[0], step_sem.at[1], device_id=sibling, device_id_type=MESH
            ).wait_send()

        if relayed:
            @pl.when(core == 0)
            def _():
                tail_pair().wait_send()

            @pl.when(core == 1)
            def _():
                pltpu.make_async_remote_copy(
                    tail_ring, tail_recv, tail_sem.at[1], tail_sem.at[0], device_id=sibling, device_id_type=MESH
                ).wait_send()

            for h, taken in enumerate(borrow):
                @pl.when(taken)
                def _():
                    forward_copy(h).wait_send()


def update(
    entries, chunks, stats, grad_ref, held,
    w_out, m_out, v_out, dir_out, drop_out, bufs, drop_ref, sems,
):
    rows, width = grad_ref.shape
    part = rows // chunks
    scale_m = jnp.concatenate([stats[8:16, :]] * (width // LANES), axis=1)
    scale_v = jnp.concatenate([stats[16:24, :]] * (width // LANES), axis=1)
    summed = jnp.sum(jnp.broadcast_to(stats[0:1, :], (SUBLANES, LANES)), axis=1, keepdims=True)
    rms = jnp.sqrt(summed * (1.0 / entries))
    clip = jnp.minimum(1.0, 0.05 / (rms + 1e-06))
    share_m, share_v = 0.1 * clip, math.sqrt(0.001) * clip
    outs = (w_out, m_out, v_out, dir_out)
    for k in range(chunks):
        at = slice(k * part, (k + 1) * part)
        grad = grad_ref[at, :]
        root = grad * share_v
        new_m = held[1, at, :] + grad * share_m
        new_v = held[2, at, :] + root * root
        weights = held[0, at, :]
        corrected = new_v * scale_v
        direction = (new_m * scale_m) / (corrected * lax.rsqrt(corrected) + 1e-08) + 0.1 * weights
        values = (weights - 0.001 * direction, new_m, new_v, direction)
        for i, (value, out) in enumerate(zip(values, outs)):
            bufs[i, at, :] = value
            pltpu.make_async_copy(bufs.at[i, pl.ds(k * part, part)], out.at[0, 0, pl.ds(k * part, part)], sems.at[i]).start()
        if k == 0:
            drop_ref[0] = jnp.max(stats[1:2, :]).astype(jnp.int32)
            drop = pltpu.make_async_copy(drop_ref, drop_out, sems.at[4])
            drop.start()
    for i, out in enumerate(outs):
        pltpu.make_async_copy(bufs.at[i], out.at[0, 0], sems.at[i]).wait()
    drop.wait()


def body(sizes, grad_parts, drop_flags, owner_order, step_count, master, moment_m, moment_v):
    n = sizes["dp"]
    chips = n // 2
    rows, columns = grad_parts.shape[-2:]
    width = master.shape[-1]
    chunks = rows // 8
    cuts = sorted({0, 8, rows - 24, rows - 8, rows})
    devices = n * sizes["tensor"] * sizes["pipe"]
    stages = [AXES] if devices <= DIRECT else [(axis,) for axis in AXES]
    peers = []
    for axes in stages:
        size = 1
        for axis in axes:
            size *= sizes[axis]
        peers.append(size - 1)
    entries = rows * columns * sizes["tensor"] * sizes["pipe"]
    padded = -(-rows // LANES) * LANES
    others = max(chips - 1, 1)
    rounds = max(sizes["pipe"] - 2, 0) + sizes["tensor"]
    f32 = jnp.float32
    dma = pltpu.SemaphoreType.DMA
    vmem = pl.BlockSpec(memory_space=pltpu.VMEM)
    hbm = pl.BlockSpec(memory_space=pltpu.HBM)
    state = jax.ShapeDtypeStruct(master.shape, f32)
    block = rows * columns * 4
    inputs = (owner_order, drop_flags.reshape(drop_flags.shape[-3:]), grad_parts, master, moment_m, moment_v)
    steps = lax.cond(
        lax.axis_index(stages[0]) == 0,
        lambda count: jnp.full((2, LANES), count.astype(f32)),
        lambda count: jnp.zeros((2, LANES), f32),
        step_count,
    )
    total, held, stats = pl.pallas_call(
        functools.partial(exchange, sizes, stages, cuts),
        out_shape=tuple(pltpu.VMEM(shape, f32) for shape in ((rows, width), (3, rows, width), (3 * SUBLANES, LANES))),
        in_specs=[vmem] + [hbm] * 6,
        out_specs=(vmem,) * 3,
        scratch_shapes=[
            pltpu.SMEM((n,), jnp.int32),
            pltpu.VMEM((1, 1, rows), jnp.int32),
            [pltpu.VMEM((n, end - start, width), f32) for start, end in zip(cuts, cuts[1:])],
            pltpu.VMEM((chips, rows, width), f32),
            pltpu.VMEM((chips, rows, width), f32),
            pltpu.VMEM((others, rows, width), f32),
            pltpu.VMEM((others, rows, width), f32),
            pltpu.VMEM((1, 1, padded), f32),
            pltpu.VMEM((n - 1, 1, padded), f32),
            [pltpu.VMEM((2, LANES), f32) for _ in peers],
            [pltpu.VMEM((max(size, 1), 2, LANES), f32) for size in peers],
            pltpu.VMEM((2, LANES), f32),
            pltpu.VMEM((2, LANES), f32),
            pltpu.VMEM((PIECES - 1, 16, width // 2), f32),
            pltpu.VMEM((2, 8, width), f32),
            pltpu.VMEM((2, 8, width), f32),
            pltpu.VMEM((2, 8, width), f32),
            dma((2,)),
            dma((len(cuts) - 1,)),
            dma((1,)),
            dma((2,)),
            dma((len(cuts),)),
            dma((1,)),
            dma((len(cuts) - 1, others)),
            dma((2,)),
            dma((len(peers), 2)),
            dma((PIECES - 1,)),
            dma((2,)),
            dma((2,)),
            pltpu.SemaphoreType.REGULAR((3,)),
            pltpu.SemaphoreType.REGULAR((rounds,)),
        ],
        compiler_params=pltpu.CompilerParams(
            collective_id=0, has_side_effects=True, vmem_limit_bytes=8 * block
        ),
        cost_estimate=pl.CostEstimate(
            flops=8 * rows * columns, bytes_accessed=20 * rows * columns * 4, transcendentals=0
        ),
    )(pltpu.with_memory_space_constraint(steps, pltpu.VMEM), *(pltpu.with_memory_space_constraint(x, pltpu.HBM) for x in inputs))
    outs = pl.pallas_call(
        functools.partial(update, entries, chunks),
        out_shape=(state, state, state, state, jax.ShapeDtypeStruct((1,), jnp.int32)),
        in_specs=[vmem] * 3,
        out_specs=(hbm,) * 5,
        scratch_shapes=[pltpu.VMEM((4, rows, width), f32), pltpu.SMEM((1,), jnp.int32), dma((5,))],
        compiler_params=pltpu.CompilerParams(vmem_limit_bytes=8 * block),
        cost_estimate=pl.CostEstimate(
            flops=20 * rows * width, bytes_accessed=8 * rows * width * 4, transcendentals=0
        ),
    )(stats, total, held)
    return (*outs[:4], outs[4].reshape(()))


def solution(mesh):
    return jax.shard_map(
        functools.partial(body, dict(mesh.shape)),
        mesh=mesh,
        in_specs=(
            P("dp", "pipe", "tensor", None, None),
            P("dp", "pipe", "tensor", None),
            P(),
            P(),
            P("pipe", "tensor", None, "dp"),
            P("pipe", "tensor", None, "dp"),
            P("pipe", "tensor", None, "dp"),
        ),
        out_specs=(
            P("pipe", "tensor", None, "dp"),
            P("pipe", "tensor", None, "dp"),
            P("pipe", "tensor", None, "dp"),
            P("pipe", "tensor", None, "dp"),
            P(),
        ),
        check_vma=False,
    )
```

```python
import functools
import itertools
import math
import jax
import jax.numpy as jnp
from jax import lax
from jax.experimental import pallas as pl
from jax.experimental.pallas import tpu as pltpu
from jax.sharding import PartitionSpec as P

AXES = ("dp", "tensor", "pipe")
MESH = pl.DeviceIdType.MESH
LANES = 128
SUBLANES = 8
DIRECT = 64
EDGES = (0, 3, 8, 11, 16)
PIECES = len(EDGES) - 1


def as_column(row, rows):
    square = (rows, rows)
    diagonal = lax.broadcasted_iota(jnp.int32, square, 0) == lax.broadcasted_iota(jnp.int32, square, 1)
    return jnp.sum(jnp.where(diagonal, jnp.broadcast_to(row, square), 0.0), axis=1, keepdims=True)


def int_power(base, exponent):
    result = jnp.ones(exponent.shape, jnp.float32)
    square = jnp.full(exponent.shape, base, jnp.float32)
    for bit in range(31):
        result = jnp.where((exponent >> bit) & 1 == 1, result * square, result)
        square = square * square
    return result


def can_relay(sizes, stages):
    return sizes["dp"] == 4 and sizes["tensor"] == 2 and len(stages) == 1 and sizes["pipe"] > 1


def exchange(
    sizes, stages, cuts,
    step_ref, order_hbm, flags_hbm, grad_hbm, w_hbm, m_hbm, v_hbm,
    total, held, stats,
    order_ref, flags_ref, g_bufs, pair_send, pair_recv, ring_send, ring_recv,
    kept_send, kept_recv, red_sends, red_recvs,
    step_send, step_recv, relay_buf, tail_send, tail_recv, tail_ring,
    o_sem, g_sem, pr_sem, rr_sem, k_sem, a_sem, via_sem, step_sem, tail_sem, chain_sem, ready_sem,
):
    n = sizes["dp"]
    chips = n // 2
    relayed = can_relay(sizes, stages)
    rows, width = total.shape
    parts = [(start, end - start) for start, end in zip(cuts, cuts[1:])]
    me = {axis: lax.axis_index(axis) for axis in AXES}
    chip, core = lax.div(me["dp"], 2), lax.rem(me["dp"], 2)

    def peer(offsets):
        return {axis: lax.rem(me[axis] + off, sizes[axis]) for axis, off in offsets.items()}

    def offsets_of(axes):
        ranges = [range(sizes[axis]) for axis in axes]
        return [dict(zip(axes, offs)) for offs in itertools.product(*ranges) if any(offs)]

    pair_sent, row_sent = o_sem.at[0], o_sem.at[1]
    ring_sent, tail_sent, held_sem, tail_paired = (g_sem.at[i] for i in range(4))
    small = [
        pltpu.make_async_copy(flags_hbm, flags_ref, o_sem.at[0]),
        pltpu.make_async_copy(order_hbm, order_ref, o_sem.at[1]),
    ]
    for copy in small:
        copy.start()
    loads = []

    def load(k):
        start, size = parts[k]
        for b in range(n):
            pltpu.make_async_copy(
                grad_hbm.at[0, 0, 0, pl.ds(start, size), pl.ds(b * width, width)], g_bufs[k].at[b], g_sem.at[k]
            ).start()
        loads.append(pltpu.make_async_copy(g_bufs[k], g_bufs[k], g_sem.at[k]))

    load(0)

    def greet(sem, axis):
        if axis == "dp":
            for off in range(1, n):
                pl.semaphore_signal(sem, inc=1, device_id=peer({"dp": off}), device_id_type=MESH)
            return n - 1
        at, last = me[axis], sizes[axis] - 1

        @pl.when(at > 0)
        def _():
            pl.semaphore_signal(sem, inc=1, device_id={**home, axis: at - 1}, device_id_type=MESH)

        @pl.when(at < last)
        def _():
            pl.semaphore_signal(sem, inc=1, device_id={**home, axis: at + 1}, device_id_type=MESH)

        return jnp.minimum(at, 1) + jnp.minimum(last - at, 1)

    sibling = {"dp": chip * 2 + 1 - core}
    barrier = pltpu.get_barrier_semaphore()

    @pl.when(core == 1)
    def _():
        pl.semaphore_signal(barrier, inc=1, device_id=sibling, device_id_type=MESH)

    home = {"dp": chip * 2 + 1}
    for off in range(1, chips):
        pl.semaphore_signal(
            barrier, inc=1, device_id={"dp": lax.rem(chip + off, chips) * 2 + 1}, device_id_type=MESH
        )
    met = 2 * (chips - 1 + greet(barrier, "tensor") + greet(barrier, "pipe"))
    home = {}
    rounds = ["pipe"] * max(sizes["pipe"] - 2, 0) + ["tensor"] * (sizes["tensor"] - 1) + ["dp"]
    left, owed = list(rounds), []

    def next_round():
        if owed:
            at, amount = owed.pop()
            pl.semaphore_wait(ready_sem.at[at], amount)
        if left:
            at = len(rounds) - len(left)
            owed.append((at, greet(ready_sem.at[at], left.pop(0))))

    load(1)

    @pl.when(core == 0)
    def _():
        pl.semaphore_wait(barrier, 1)
        pl.semaphore_signal(chain_sem.at[2], inc=1, device_id=sibling, device_id_type=MESH)

    for copy in small:
        copy.wait()
    for k in range(2, len(parts)):
        load(k)
    flags_row = flags_ref[0].astype(jnp.float32)
    kept_row = 1.0 - flags_row
    kept = as_column(kept_row, rows)
    kept_send[0, :, 0:rows] = kept_row
    dropped = jnp.sum(flags_row, axis=1, keepdims=True)

    def chip_at(slot):
        return lax.rem(chip + slot, chips)

    def term(k, owner):
        start, size = parts[k]
        return g_bufs[k][order_ref[owner]] * kept[start:start + size]

    def rows_of(ref, slot, k):
        start, size = parts[k]
        return ref.at[slot, pl.ds(start, size)]

    pair = {}

    def send_pair(k, slot):
        copy = pltpu.make_async_remote_copy(
            rows_of(pair_send, slot, k), rows_of(pair_recv, slot, k),
            pair_sent, pr_sem.at[k if slot else pr_sem.shape[0] - 1],
            device_id=sibling, device_id_type=MESH,
        )
        copy.start()
        pair[k, slot] = copy

    far = list(range(1, chips))
    def to_sibling(k):
        start, size = parts[k]
        with jax.named_scope(f"load_wait{k}"):
            loads[k].wait()
        for slot in far:
            pair_send[slot, start:start + size, :] = term(k, chip_at(slot) * 2 + 1 - core)
        if k == 0:
            with jax.named_scope("sibling_wait"):
                @pl.when(core == 1)
                def _():
                    pl.semaphore_wait(chain_sem.at[2], 1)
        for slot in far:
            send_pair(k, slot)

    kepts = pltpu.make_async_remote_copy(
        kept_recv, kept_recv, row_sent, k_sem.at[0], device_id=sibling, device_id_type=MESH
    )

    ring = {}
    swing = len(parts) - 2
    far_end = sizes["pipe"] - 1
    gap = 2 * me["pipe"] - far_end
    across = {"dp": chip_at(1) * 2 + core}
    lend = [gap >= 1, gap >= 3, 2 * me["tensor"] >= sizes["tensor"]] if relayed else []
    borrow = [gap <= -1, gap <= -3, 2 * me["tensor"] < sizes["tensor"]] if relayed else []
    mirror = [{"pipe": far_end - me["pipe"]}] * 2 + [{"tensor": sizes["tensor"] - 1 - me["tensor"]}]
    edges = [width * edge // 16 for edge in EDGES]

    def piece(ref, h):
        start, size = parts[swing]
        return ref.at[0, pl.ds(start, size), pl.ds(edges[h], edges[h + 1] - edges[h])]

    def lodging(h):
        return relay_buf.at[h, :, pl.ds(0, edges[h + 1] - edges[h])]

    def swing_copy(h):
        return pltpu.make_async_remote_copy(
            piece(ring_send, h), piece(ring_recv, h), ring_sent, rr_sem.at[swing, 0],
            device_id=across, device_id_type=MESH,
        )

    def via_copy(h):
        return pltpu.make_async_remote_copy(
            piece(ring_send, h), lodging(h), ring_sent, via_sem.at[h],
            device_id={**across, **mirror[h]}, device_id_type=MESH,
        )

    def forward_copy(h):
        return pltpu.make_async_remote_copy(
            lodging(h), piece(ring_recv, h), via_sem.at[h], rr_sem.at[swing, 0],
            device_id=mirror[h], device_id_type=MESH,
        )

    def climb():
        at = me["pipe"]

        @pl.when(at >= 2)
        def _():
            pl.semaphore_wait(chain_sem.at[0], 1)

        @pl.when((at >= 1) & (at < far_end))
        def _():
            pl.semaphore_signal(chain_sem.at[0], inc=1, device_id={"pipe": at + 1}, device_id_type=MESH)

        @pl.when(lend[0] | lend[2])
        def _():
            pl.semaphore_signal(chain_sem.at[1], inc=1, device_id=across, device_id_type=MESH)

    tail = len(parts) - 1
    tail_at = pl.ds(*parts[tail])
    abroad = chip_at(1) * 2

    def tail_pair():
        return pltpu.make_async_remote_copy(
            tail_send, tail_recv, tail_paired, tail_sem.at[0], device_id=sibling, device_id_type=MESH
        )

    def tail_copy(c):
        return pltpu.make_async_remote_copy(
            tail_ring.at[c], ring_recv.at[0, tail_at], tail_sent, rr_sem.at[tail, 0],
            device_id={"dp": abroad + c}, device_id_type=MESH,
        )

    def tail_to_sibling():
        loads[tail].wait()

        @pl.when(core == 0)
        def _():
            for c in range(2):
                tail_send[c] = term(tail, abroad + c)
            tail_pair().start()

    def tail_to_owner():
        @pl.when(core == 1)
        def _():
            tail_pair().wait_recv()
            for c in range(2):
                tail_ring[c] = tail_recv[c] + term(tail, abroad + c)
                tail_copy(c).start()

    def to_owner(k):
        start, size = parts[k]
        for slot in far:
            target = chip_at(slot) * 2 + core
            mine = term(k, target)
            with jax.named_scope(f"pair_wait{k}"):
                if slot == far[0]:
                    pltpu.make_async_remote_copy(
                        pair_recv.at[pl.ds(1, chips - 1), pl.ds(start, size)],
                        pair_recv.at[pl.ds(1, chips - 1), pl.ds(start, size)],
                        pair_sent, pr_sem.at[k], device_id=sibling, device_id_type=MESH,
                    ).wait_recv()
            ring_send[slot - 1, start:start + size, :] = pair_recv[slot, start:start + size, :] + mine
            if relayed and k == swing:
                @pl.when(lend[0] | lend[2])
                def _():
                    with jax.named_scope("chain_wait"):
                        pl.semaphore_wait(chain_sem.at[1], 1)

                for h, away in enumerate(lend):
                    @pl.when(away)
                    def _():
                        via_copy(h).start()

                for h, away in enumerate(lend):
                    @pl.when(jnp.logical_not(away))
                    def _():
                        swing_copy(h).start()
                for h in range(len(lend), PIECES):
                    swing_copy(h).start()
                continue
            copy = pltpu.make_async_remote_copy(
                rows_of(ring_send, slot - 1, k), rows_of(ring_recv, slot - 1, k),
                ring_sent, rr_sem.at[k, slot - 1],
                device_id={"dp": target}, device_id_type=MESH,
            )
            copy.start()
            ring[k, slot] = copy

    to_sibling(0)
    to_sibling(1)
    with jax.named_scope("barrier_wait"):
        @pl.when(core == 1)
        def _():
            pl.semaphore_wait(barrier, met)
            pl.semaphore_signal(chain_sem.at[2], inc=1, device_id=sibling, device_id_type=MESH)

        @pl.when(core == 0)
        def _():
            pl.semaphore_wait(chain_sem.at[2], 1)
    for off in range(1, n):
        pltpu.make_async_remote_copy(
            kept_send.at[0], kept_recv.at[off - 1], row_sent, k_sem.at[0],
            device_id=peer({"dp": off}), device_id_type=MESH,
        ).start()
    to_owner(0)
    if relayed:
        climb()
    else:
        to_owner(1)
    if relayed:
        tail_to_sibling()
        to_sibling(swing)
        to_owner(1)
        tail_to_owner()
        to_owner(swing)
    else:
        for k in range(2, len(parts)):
            to_sibling(k)
        for k in range(2, len(parts)):
            to_owner(k)

    next_round()
    sent = pl.ds(0, parts[tail][0] if relayed else rows)
    slots = pl.ds(0, chips - 1)
    if far:
        pltpu.make_async_remote_copy(
            ring_send.at[slots, sent], ring_recv.at[slots, sent], pair_sent, pr_sem.at[0],
            device_id=sibling, device_id_type=MESH,
        ).wait_send()
    for k, (start, size) in enumerate(parts):
        pair_send[0, start:start + size, :] = term(k, chip * 2 + 1 - core)
        send_pair(k, 0)
    with jax.named_scope("kept_wait"):
        kepts.wait_recv()
    kepts.wait_send()
    count_row = kept_row
    for i in range(n - 1):
        count_row = count_row + kept_recv[i, :, 0:rows]
    inverse = 1.0 / jnp.maximum(as_column(count_row, rows), 1.0)
    next_round()
    for i, source in enumerate((w_hbm, m_hbm, v_hbm)):
        pltpu.make_async_copy(source.at[0, 0], held.at[i], held_sem).start()

    pltpu.make_async_remote_copy(
        pair_recv.at[0], pair_recv.at[0], pair_sent, pr_sem.at[pr_sem.shape[0] - 1],
        device_id=sibling, device_id_type=MESH,
    ).wait_recv()
    for k, (start, size) in enumerate(parts):
        total[start:start + size, :] = pair_recv[0, start:start + size, :] + term(k, me["dp"])
    pltpu.make_async_copy(held, held, held_sem).wait()
    held[1] = 0.9 * held[1]
    held[2] = 0.999 * held[2]
    next_round()

    if relayed:
        for h in (2, 0, 1):
            @pl.when(borrow[h])
            def _():
                with jax.named_scope(f"relay_wait{h}"):
                    via_copy(h).wait_recv()
                forward_copy(h).start()

    while left or owed:
        next_round()
    first = functools.reduce(jnp.logical_and, [me[axis] == 0 for axis in stages[0]])

    def tell(device):
        return pltpu.make_async_remote_copy(
            step_send, step_recv, row_sent, step_sem.at[0], device_id=device, device_id_type=MESH
        )

    @pl.when(first)
    def _():
        step_send[...] = step_ref[...]
        step_recv[...] = step_ref[...]
        for off in offsets_of(stages[0]):
            tell(off).start()

    squares = jnp.zeros((SUBLANES, LANES), jnp.float32)
    for k in [i for i in range(len(parts)) if not relayed or i != swing] + [swing] * relayed:
        start, size = parts[k]
        at = slice(start, start + size)
        value = total[at, :]
        for slot in far:
            with jax.named_scope(f"ring_wait{k}"):
                if relayed and k == swing:
                    pltpu.make_async_remote_copy(
                        ring_recv.at[0, pl.ds(start, size)], ring_recv.at[0, pl.ds(start, size)],
                        ring_sent, rr_sem.at[swing, 0], device_id=across, device_id_type=MESH,
                    ).wait_recv()
                elif relayed and k == tail:
                    tail_copy(0).wait_recv()
                else:
                    ring[k, slot].wait_recv()
            value = value + ring_recv[slot - 1, at, :]
        value = value * inverse[at]
        total[at, :] = value
        squares = squares + jnp.sum(
            (value * value).reshape(size // SUBLANES, SUBLANES, width // LANES, LANES), axis=(0, 2)
        )

    @pl.when(first)
    def _():
        pltpu.make_async_remote_copy(
            red_recvs[0], red_recvs[0], row_sent, step_sem.at[0], device_id=sibling, device_id_type=MESH
        ).wait_send()

    result = [jnp.sum(squares, axis=0, keepdims=True), jnp.broadcast_to(dropped, (1, LANES))]
    for stage, (axes, send, recv) in enumerate(zip(stages, red_sends, red_recvs)):
        for i, row in enumerate(result):
            send[i:i + 1, :] = row
        with jax.named_scope("norm_send"):
            back, stride = 0, 1
            for axis in reversed(axes):
                back, stride = back + lax.rem(sizes[axis] - me[axis], sizes[axis]) * stride, stride * sizes[axis]

            def share(i, device):
                pltpu.make_async_remote_copy(
                    send, recv.at[i], row_sent, a_sem.at[stage],
                    device_id=device, device_id_type=MESH,
                ).start()

            @pl.when(back > 0)
            def _():
                share(back - 1, dict.fromkeys(axes, 0))

            for i, off in enumerate(offsets_of(axes)):
                @pl.when(back != i + 1)
                def _():
                    share(i, peer(off))
        if stage == 0:
            @pl.when(jnp.logical_not(first))
            def _():
                tell(sibling).wait_recv()

            steps = jnp.broadcast_to(step_recv[0:1, :], (SUBLANES, LANES)).astype(jnp.int32)
            stats[0:8, :] = jnp.zeros((SUBLANES, LANES), jnp.float32)
            stats[8:16, :] = 1.0 / (1.0 - int_power(0.9, steps))
            stats[16:24, :] = 1.0 / (1.0 - int_power(0.999, steps))
        copy = pltpu.make_async_remote_copy(
            recv, recv, row_sent, a_sem.at[stage], device_id=sibling, device_id_type=MESH
        )
        with jax.named_scope("norm_wait"):
            copy.wait_recv()
        copy.wait_send()
        for i in range(len(offsets_of(axes))):
            result = [row + recv[i, j:j + 1, :] for j, row in enumerate(result)]
    for i, row in enumerate(result):
        stats[i:i + 1, :] = row

    with jax.named_scope("send_wait"):
        pltpu.make_async_remote_copy(
            pair_send.at[0], pair_recv.at[0], pair_sent, pr_sem.at[0], device_id=sibling, device_id_type=MESH
        ).wait_send()
        if far:
            pltpu.make_async_remote_copy(
                ring_send.at[slots, sent], ring_recv.at[slots, sent], ring_sent, rr_sem.at[0, 0],
                device_id=sibling, device_id_type=MESH,
            ).wait_send()
        if relayed:
            @pl.when(core == 0)
            def _():
                tail_pair().wait_send()

            @pl.when(core == 1)
            def _():
                pltpu.make_async_remote_copy(
                    tail_ring, tail_recv, tail_sent, tail_sem.at[0], device_id=sibling, device_id_type=MESH
                ).wait_send()

            for h, taken in enumerate(borrow):
                @pl.when(taken)
                def _():
                    forward_copy(h).wait_send()


def update(
    entries, chunks, stats, grad_ref, held,
    w_out, m_out, v_out, dir_out, drop_out, bufs, drop_ref, sems,
):
    rows, width = grad_ref.shape
    part = rows // chunks
    scale_m = jnp.concatenate([stats[8:16, :]] * (width // LANES), axis=1)
    scale_v = jnp.concatenate([stats[16:24, :]] * (width // LANES), axis=1)
    summed = jnp.sum(jnp.broadcast_to(stats[0:1, :], (SUBLANES, LANES)), axis=1, keepdims=True)
    rms = jnp.sqrt(summed * (1.0 / entries))
    clip = jnp.minimum(1.0, 0.05 / (rms + 1e-06))
    share_m, share_v = 0.1 * clip, math.sqrt(0.001) * clip
    outs = (w_out, m_out, v_out, dir_out)

    def put(i, k, value):
        bufs[i, k * part:(k + 1) * part, :] = value
        rows_of = pl.ds(k * part, part)
        pltpu.make_async_copy(bufs.at[i, rows_of], outs[i].at[0, 0, rows_of], sems.at[i]).start()

    for k in range(chunks):
        at = slice(k * part, (k + 1) * part)
        grad = grad_ref[at, :]
        root = grad * share_v
        put(1, k, held[1, at, :] + grad * share_m)
        put(2, k, held[2, at, :] + root * root)
    for k in range(chunks):
        at = slice(k * part, (k + 1) * part)
        weights = held[0, at, :]
        corrected = bufs[2, at, :] * scale_v
        direction = (bufs[1, at, :] * scale_m) / (corrected * lax.rsqrt(corrected) + 1e-08) + 0.1 * weights
        put(3, k, direction)
        put(0, k, weights - 0.001 * direction)
        if k == 0:
            drop_ref[0] = jnp.max(stats[1:2, :]).astype(jnp.int32)
            drop = pltpu.make_async_copy(drop_ref, drop_out, sems.at[4])
            drop.start()
    for i, out in enumerate(outs):
        pltpu.make_async_copy(bufs.at[i], out.at[0, 0], sems.at[i]).wait()
    drop.wait()


def body(sizes, grad_parts, drop_flags, owner_order, step_count, master, moment_m, moment_v):
    n = sizes["dp"]
    chips = n // 2
    rows, columns = grad_parts.shape[-2:]
    width = master.shape[-1]
    chunks = rows // 8
    cuts = sorted({0, 8, rows - 24, rows - 8, rows})
    devices = n * sizes["tensor"] * sizes["pipe"]
    stages = [AXES] if devices <= DIRECT else [(axis,) for axis in AXES]
    peers = []
    for axes in stages:
        size = 1
        for axis in axes:
            size *= sizes[axis]
        peers.append(size - 1)
    entries = rows * columns * sizes["tensor"] * sizes["pipe"]
    padded = -(-rows // LANES) * LANES
    others = max(chips - 1, 1)
    rounds = max(sizes["pipe"] - 2, 0) + sizes["tensor"]
    f32 = jnp.float32
    dma = pltpu.SemaphoreType.DMA
    vmem = pl.BlockSpec(memory_space=pltpu.VMEM)
    hbm = pl.BlockSpec(memory_space=pltpu.HBM)
    state = jax.ShapeDtypeStruct(master.shape, f32)
    block = rows * columns * 4
    inputs = (owner_order, drop_flags.reshape(drop_flags.shape[-3:]), grad_parts, master, moment_m, moment_v)
    steps = lax.cond(
        lax.axis_index(stages[0]) == 0,
        lambda count: jnp.full((2, LANES), count.astype(f32)),
        lambda count: jnp.zeros((2, LANES), f32),
        step_count,
    )
    total, held, stats = pl.pallas_call(
        functools.partial(exchange, sizes, stages, cuts),
        out_shape=tuple(pltpu.VMEM(shape, f32) for shape in ((rows, width), (3, rows, width), (3 * SUBLANES, LANES))),
        in_specs=[vmem] + [hbm] * 6,
        out_specs=(vmem,) * 3,
        scratch_shapes=[
            pltpu.SMEM((n,), jnp.int32),
            pltpu.VMEM((1, 1, rows), jnp.int32),
            [pltpu.VMEM((n, end - start, width), f32) for start, end in zip(cuts, cuts[1:])],
            pltpu.VMEM((chips, rows, width), f32),
            pltpu.VMEM((chips, rows, width), f32),
            pltpu.VMEM((others, rows, width), f32),
            pltpu.VMEM((others, rows, width), f32),
            pltpu.VMEM((1, 1, padded), f32),
            pltpu.VMEM((n - 1, 1, padded), f32),
            [pltpu.VMEM((2, LANES), f32) for _ in peers],
            [pltpu.VMEM((max(size, 1), 2, LANES), f32) for size in peers],
            pltpu.VMEM((2, LANES), f32),
            pltpu.VMEM((2, LANES), f32),
            pltpu.VMEM((PIECES - 1, 16, width // 2), f32),
            pltpu.VMEM((2, 8, width), f32),
            pltpu.VMEM((2, 8, width), f32),
            pltpu.VMEM((2, 8, width), f32),
            dma((2,)),
            dma((max(len(cuts) - 1, 4),)),
            dma((len(cuts) - 1 if can_relay(sizes, stages) else len(cuts),)),
            dma((len(cuts) - 1, others)),
            dma((1,)),
            dma((len(peers),)),
            dma((PIECES - 1,)),
            dma((1,)),
            dma((1,)),
            pltpu.SemaphoreType.REGULAR((3,)),
            pltpu.SemaphoreType.REGULAR((rounds,)),
        ],
        compiler_params=pltpu.CompilerParams(
            collective_id=0, has_side_effects=True, vmem_limit_bytes=8 * block
        ),
        cost_estimate=pl.CostEstimate(
            flops=8 * rows * columns, bytes_accessed=20 * rows * columns * 4, transcendentals=0
        ),
    )(pltpu.with_memory_space_constraint(steps, pltpu.VMEM), *(pltpu.with_memory_space_constraint(x, pltpu.HBM) for x in inputs))
    outs = pl.pallas_call(
        functools.partial(update, entries, chunks),
        out_shape=(state, state, state, state, jax.ShapeDtypeStruct((1,), jnp.int32)),
        in_specs=[vmem] * 3,
        out_specs=(hbm,) * 5,
        scratch_shapes=[pltpu.VMEM((4, rows, width), f32), pltpu.SMEM((1,), jnp.int32), dma((5,))],
        compiler_params=pltpu.CompilerParams(vmem_limit_bytes=8 * block),
        cost_estimate=pl.CostEstimate(
            flops=20 * rows * width, bytes_accessed=8 * rows * width * 4, transcendentals=0
        ),
    )(stats, total, held)
    return (*outs[:4], outs[4].reshape(()))


def solution(mesh):
    return jax.shard_map(
        functools.partial(body, dict(mesh.shape)),
        mesh=mesh,
        in_specs=(
            P("dp", "pipe", "tensor", None, None),
            P("dp", "pipe", "tensor", None),
            P(),
            P(),
            P("pipe", "tensor", None, "dp"),
            P("pipe", "tensor", None, "dp"),
            P("pipe", "tensor", None, "dp"),
        ),
        out_specs=(
            P("pipe", "tensor", None, "dp"),
            P("pipe", "tensor", None, "dp"),
            P("pipe", "tensor", None, "dp"),
            P("pipe", "tensor", None, "dp"),
            P(),
        ),
        check_vma=False,
    )
```

```python
import functools
import itertools
import math
import jax
import jax.numpy as jnp
from jax import lax
from jax.experimental import pallas as pl
from jax.experimental.pallas import tpu as pltpu
from jax.sharding import PartitionSpec as P

AXES = ("dp", "tensor", "pipe")
MESH = pl.DeviceIdType.MESH
LANES = 128
SUBLANES = 8
DIRECT = 64
EDGES = (0, 3, 8, 11, 16)
PIECES = len(EDGES) - 1


def as_column(row, rows):
    square = (rows, rows)
    diagonal = lax.broadcasted_iota(jnp.int32, square, 0) == lax.broadcasted_iota(jnp.int32, square, 1)
    return jnp.sum(jnp.where(diagonal, jnp.broadcast_to(row, square), 0.0), axis=1, keepdims=True)


def int_power(base, exponent):
    result = jnp.ones(exponent.shape, jnp.float32)
    square = jnp.full(exponent.shape, base, jnp.float32)
    for bit in range(31):
        result = jnp.where((exponent >> bit) & 1 == 1, result * square, result)
        square = square * square
    return result


def can_relay(sizes, stages):
    return sizes["dp"] == 4 and sizes["tensor"] == 2 and len(stages) == 1 and sizes["pipe"] > 1


def exchange(
    sizes, stages, cuts,
    step_ref, order_hbm, flags_hbm, grad_hbm, w_hbm, m_hbm, v_hbm,
    total, held, stats,
    order_ref, flags_ref, g_bufs, pair_send, pair_recv, ring_send, ring_recv,
    kept_send, kept_recv, red_sends, red_recvs,
    step_send, step_recv, relay_buf, tail_send, tail_recv, tail_ring,
    o_sem, g_sem, pr_sem, rr_sem, k_sem, a_sem, via_sem, step_sem, tail_sem, chain_sem, ready_sem,
):
    n = sizes["dp"]
    chips = n // 2
    relayed = can_relay(sizes, stages)
    rows, width = total.shape
    parts = [(start, end - start) for start, end in zip(cuts, cuts[1:])]
    me = {axis: lax.axis_index(axis) for axis in AXES}
    chip, core = lax.div(me["dp"], 2), lax.rem(me["dp"], 2)

    def peer(offsets):
        return {axis: lax.rem(me[axis] + off, sizes[axis]) for axis, off in offsets.items()}

    def offsets_of(axes):
        ranges = [range(sizes[axis]) for axis in axes]
        return [dict(zip(axes, offs)) for offs in itertools.product(*ranges) if any(offs)]

    pair_sent, row_sent = o_sem.at[0], o_sem.at[1]
    ring_sent, tail_sent, held_sem, tail_paired = (g_sem.at[i] for i in range(4))
    small = [
        pltpu.make_async_copy(flags_hbm, flags_ref, o_sem.at[0]),
        pltpu.make_async_copy(order_hbm, order_ref, o_sem.at[1]),
    ]
    for copy in small:
        copy.start()
    loads = []

    def load(k):
        start, size = parts[k]
        for b in range(n):
            pltpu.make_async_copy(
                grad_hbm.at[0, 0, 0, pl.ds(start, size), pl.ds(b * width, width)], g_bufs[k].at[b], g_sem.at[k]
            ).start()
        loads.append(pltpu.make_async_copy(g_bufs[k], g_bufs[k], g_sem.at[k]))

    load(0)

    def greet(sem, axis):
        if axis == "dp":
            for off in range(1, n):
                pl.semaphore_signal(sem, inc=1, device_id=peer({"dp": off}), device_id_type=MESH)
            return n - 1
        at, last = me[axis], sizes[axis] - 1

        @pl.when(at > 0)
        def _():
            pl.semaphore_signal(sem, inc=1, device_id={**home, axis: at - 1}, device_id_type=MESH)

        @pl.when(at < last)
        def _():
            pl.semaphore_signal(sem, inc=1, device_id={**home, axis: at + 1}, device_id_type=MESH)

        return jnp.minimum(at, 1) + jnp.minimum(last - at, 1)

    sibling = {"dp": chip * 2 + 1 - core}
    barrier = pltpu.get_barrier_semaphore()

    @pl.when(core == 1)
    def _():
        pl.semaphore_signal(barrier, inc=1, device_id=sibling, device_id_type=MESH)

    home = {"dp": chip * 2 + 1}
    for off in range(1, chips):
        pl.semaphore_signal(
            barrier, inc=1, device_id={"dp": lax.rem(chip + off, chips) * 2 + 1}, device_id_type=MESH
        )
    met = 2 * (chips - 1 + greet(barrier, "tensor") + greet(barrier, "pipe"))
    home = {}
    rounds = ["pipe"] * max(sizes["pipe"] - 2, 0) + ["tensor"] * (sizes["tensor"] - 1) + ["dp"]
    left, owed = list(rounds), []

    def next_round():
        if owed:
            at, amount = owed.pop()
            pl.semaphore_wait(ready_sem.at[at], amount)
        if left:
            at = len(rounds) - len(left)
            owed.append((at, greet(ready_sem.at[at], left.pop(0))))

    load(1)

    @pl.when(core == 0)
    def _():
        pl.semaphore_wait(barrier, 1)
        pl.semaphore_signal(chain_sem.at[2], inc=1, device_id=sibling, device_id_type=MESH)

    for copy in small:
        copy.wait()
    for k in range(2, len(parts)):
        load(k)
    flags_row = flags_ref[0].astype(jnp.float32)
    kept_row = 1.0 - flags_row
    kept = as_column(kept_row, rows)
    kept_send[0, :, 0:rows] = kept_row
    dropped = jnp.sum(flags_row, axis=1, keepdims=True)

    def chip_at(slot):
        return lax.rem(chip + slot, chips)

    def term(k, owner):
        start, size = parts[k]
        return g_bufs[k][order_ref[owner]] * kept[start:start + size]

    def rows_of(ref, slot, k):
        start, size = parts[k]
        return ref.at[slot, pl.ds(start, size)]

    pair = {}

    def send_pair(k, slot):
        copy = pltpu.make_async_remote_copy(
            rows_of(pair_send, slot, k), rows_of(pair_recv, slot, k),
            pair_sent, pr_sem.at[k if slot else pr_sem.shape[0] - 1],
            device_id=sibling, device_id_type=MESH,
        )
        copy.start()
        pair[k, slot] = copy

    far = list(range(1, chips))
    def to_sibling(k):
        start, size = parts[k]
        with jax.named_scope(f"load_wait{k}"):
            loads[k].wait()
        for slot in far:
            pair_send[slot, start:start + size, :] = term(k, chip_at(slot) * 2 + 1 - core)
        if k == 0:
            with jax.named_scope("sibling_wait"):
                @pl.when(core == 1)
                def _():
                    pl.semaphore_wait(chain_sem.at[2], 1)
        for slot in far:
            send_pair(k, slot)

    kepts = pltpu.make_async_remote_copy(
        kept_recv, kept_recv, row_sent, k_sem.at[0], device_id=sibling, device_id_type=MESH
    )

    ring = {}
    swing = len(parts) - 2
    far_end = sizes["pipe"] - 1
    gap = 2 * me["pipe"] - far_end
    across = {"dp": chip_at(1) * 2 + core}
    lend = [gap >= 1, gap >= 3, 2 * me["tensor"] >= sizes["tensor"]] if relayed else []
    borrow = [gap <= -1, gap <= -3, 2 * me["tensor"] < sizes["tensor"]] if relayed else []
    mirror = [{"pipe": far_end - me["pipe"]}] * 2 + [{"tensor": sizes["tensor"] - 1 - me["tensor"]}]
    edges = [width * edge // 16 for edge in EDGES]

    def piece(ref, h):
        start, size = parts[swing]
        return ref.at[0, pl.ds(start, size), pl.ds(edges[h], edges[h + 1] - edges[h])]

    def lodging(h):
        return relay_buf.at[h, :, pl.ds(0, edges[h + 1] - edges[h])]

    def swing_copy(h):
        return pltpu.make_async_remote_copy(
            piece(ring_send, h), piece(ring_recv, h), ring_sent, rr_sem.at[swing, 0],
            device_id=across, device_id_type=MESH,
        )

    def via_copy(h):
        return pltpu.make_async_remote_copy(
            piece(ring_send, h), lodging(h), ring_sent, via_sem.at[h],
            device_id={**across, **mirror[h]}, device_id_type=MESH,
        )

    def forward_copy(h):
        return pltpu.make_async_remote_copy(
            lodging(h), piece(ring_recv, h), via_sem.at[h], rr_sem.at[swing, 0],
            device_id=mirror[h], device_id_type=MESH,
        )

    def climb():
        at = me["pipe"]

        @pl.when(at >= 2)
        def _():
            pl.semaphore_wait(chain_sem.at[0], 1)

        @pl.when((at >= 1) & (at < far_end))
        def _():
            pl.semaphore_signal(chain_sem.at[0], inc=1, device_id={"pipe": at + 1}, device_id_type=MESH)

        @pl.when(lend[0] | lend[2])
        def _():
            pl.semaphore_signal(chain_sem.at[1], inc=1, device_id=across, device_id_type=MESH)

    tail = len(parts) - 1
    tail_at = pl.ds(*parts[tail])
    abroad = chip_at(1) * 2

    def tail_pair():
        return pltpu.make_async_remote_copy(
            tail_send, tail_recv, tail_paired, tail_sem.at[0], device_id=sibling, device_id_type=MESH
        )

    def tail_copy(c):
        return pltpu.make_async_remote_copy(
            tail_ring.at[c], ring_recv.at[0, tail_at], tail_sent, rr_sem.at[tail, 0],
            device_id={"dp": abroad + c}, device_id_type=MESH,
        )

    def tail_to_sibling():
        loads[tail].wait()

        @pl.when(core == 0)
        def _():
            for c in range(2):
                tail_send[c] = term(tail, abroad + c)
            tail_pair().start()

    def tail_to_owner():
        @pl.when(core == 1)
        def _():
            tail_pair().wait_recv()
            for c in range(2):
                tail_ring[c] = tail_recv[c] + term(tail, abroad + c)
                tail_copy(c).start()

    def to_owner(k):
        start, size = parts[k]
        for slot in far:
            target = chip_at(slot) * 2 + core
            mine = term(k, target)
            with jax.named_scope(f"pair_wait{k}"):
                if slot == far[0]:
                    pltpu.make_async_remote_copy(
                        pair_recv.at[pl.ds(1, chips - 1), pl.ds(start, size)],
                        pair_recv.at[pl.ds(1, chips - 1), pl.ds(start, size)],
                        pair_sent, pr_sem.at[k], device_id=sibling, device_id_type=MESH,
                    ).wait_recv()
            ring_send[slot - 1, start:start + size, :] = pair_recv[slot, start:start + size, :] + mine
            if relayed and k == swing:
                @pl.when(lend[0] | lend[2])
                def _():
                    with jax.named_scope("chain_wait"):
                        pl.semaphore_wait(chain_sem.at[1], 1)

                for h, away in enumerate(lend):
                    @pl.when(away)
                    def _():
                        via_copy(h).start()

                for h, away in enumerate(lend):
                    @pl.when(jnp.logical_not(away))
                    def _():
                        swing_copy(h).start()
                for h in range(len(lend), PIECES):
                    swing_copy(h).start()
                continue
            copy = pltpu.make_async_remote_copy(
                rows_of(ring_send, slot - 1, k), rows_of(ring_recv, slot - 1, k),
                ring_sent, rr_sem.at[k, slot - 1],
                device_id={"dp": target}, device_id_type=MESH,
            )
            copy.start()
            ring[k, slot] = copy

    to_sibling(0)
    to_sibling(1)
    with jax.named_scope("barrier_wait"):
        @pl.when(core == 1)
        def _():
            pl.semaphore_wait(barrier, met)
            pl.semaphore_signal(chain_sem.at[2], inc=1, device_id=sibling, device_id_type=MESH)

        @pl.when(core == 0)
        def _():
            pl.semaphore_wait(chain_sem.at[2], 1)
    for off in range(1, n):
        pltpu.make_async_remote_copy(
            kept_send.at[0], kept_recv.at[off - 1], row_sent, k_sem.at[0],
            device_id=peer({"dp": off}), device_id_type=MESH,
        ).start()
    to_owner(0)
    if relayed:
        climb()
    else:
        to_owner(1)
    if relayed:
        to_sibling(swing)
        tail_to_sibling()
        to_owner(1)
        tail_to_owner()
        to_owner(swing)
    else:
        for k in range(2, len(parts)):
            to_sibling(k)
        for k in range(2, len(parts)):
            to_owner(k)

    next_round()
    sent = pl.ds(0, parts[tail][0] if relayed else rows)
    slots = pl.ds(0, chips - 1)
    if far:
        pltpu.make_async_remote_copy(
            ring_send.at[slots, sent], ring_recv.at[slots, sent], pair_sent, pr_sem.at[0],
            device_id=sibling, device_id_type=MESH,
        ).wait_send()
    for k, (start, size) in enumerate(parts):
        pair_send[0, start:start + size, :] = term(k, chip * 2 + 1 - core)
        send_pair(k, 0)
    with jax.named_scope("kept_wait"):
        kepts.wait_recv()
    kepts.wait_send()
    count_row = kept_row
    for i in range(n - 1):
        count_row = count_row + kept_recv[i, :, 0:rows]
    inverse = 1.0 / jnp.maximum(as_column(count_row, rows), 1.0)
    next_round()
    for i, source in enumerate((w_hbm, m_hbm, v_hbm)):
        pltpu.make_async_copy(source.at[0, 0], held.at[i], held_sem).start()

    pltpu.make_async_remote_copy(
        pair_recv.at[0], pair_recv.at[0], pair_sent, pr_sem.at[pr_sem.shape[0] - 1],
        device_id=sibling, device_id_type=MESH,
    ).wait_recv()
    for k, (start, size) in enumerate(parts):
        total[start:start + size, :] = pair_recv[0, start:start + size, :] + term(k, me["dp"])
    pltpu.make_async_copy(held, held, held_sem).wait()
    held[1] = 0.9 * held[1]
    held[2] = 0.999 * held[2]
    next_round()

    if relayed:
        for h in (2, 0, 1):
            @pl.when(borrow[h])
            def _():
                with jax.named_scope(f"relay_wait{h}"):
                    via_copy(h).wait_recv()
                forward_copy(h).start()

    while left or owed:
        next_round()
    first = functools.reduce(jnp.logical_and, [me[axis] == 0 for axis in stages[0]])

    def tell(device):
        return pltpu.make_async_remote_copy(
            step_send, step_recv, row_sent, step_sem.at[0], device_id=device, device_id_type=MESH
        )

    @pl.when(first)
    def _():
        step_send[...] = step_ref[...]
        step_recv[...] = step_ref[...]
        for off in offsets_of(stages[0]):
            tell(off).start()

    squares = jnp.zeros((SUBLANES, LANES), jnp.float32)
    for k in [i for i in range(len(parts)) if not relayed or i != swing] + [swing] * relayed:
        start, size = parts[k]
        at = slice(start, start + size)
        value = total[at, :]
        for slot in far:
            with jax.named_scope(f"ring_wait{k}"):
                if relayed and k == swing:
                    pltpu.make_async_remote_copy(
                        ring_recv.at[0, pl.ds(start, size)], ring_recv.at[0, pl.ds(start, size)],
                        ring_sent, rr_sem.at[swing, 0], device_id=across, device_id_type=MESH,
                    ).wait_recv()
                elif relayed and k == tail:
                    tail_copy(0).wait_recv()
                else:
                    ring[k, slot].wait_recv()
            value = value + ring_recv[slot - 1, at, :]
        value = value * inverse[at]
        total[at, :] = value
        squares = squares + jnp.sum(
            (value * value).reshape(size // SUBLANES, SUBLANES, width // LANES, LANES), axis=(0, 2)
        )

    @pl.when(first)
    def _():
        pltpu.make_async_remote_copy(
            red_recvs[0], red_recvs[0], row_sent, step_sem.at[0], device_id=sibling, device_id_type=MESH
        ).wait_send()

    result = [jnp.sum(squares, axis=0, keepdims=True), jnp.broadcast_to(dropped, (1, LANES))]
    for stage, (axes, send, recv) in enumerate(zip(stages, red_sends, red_recvs)):
        for i, row in enumerate(result):
            send[i:i + 1, :] = row
        with jax.named_scope("norm_send"):
            back, stride = 0, 1
            for axis in reversed(axes):
                back, stride = back + lax.rem(sizes[axis] - me[axis], sizes[axis]) * stride, stride * sizes[axis]

            def share(i, device):
                pltpu.make_async_remote_copy(
                    send, recv.at[i], row_sent, a_sem.at[stage],
                    device_id=device, device_id_type=MESH,
                ).start()

            @pl.when(back > 0)
            def _():
                share(back - 1, dict.fromkeys(axes, 0))

            for i, off in enumerate(offsets_of(axes)):
                @pl.when(back != i + 1)
                def _():
                    share(i, peer(off))
        if stage == 0:
            @pl.when(jnp.logical_not(first))
            def _():
                tell(sibling).wait_recv()

            steps = jnp.broadcast_to(step_recv[0:1, :], (SUBLANES, LANES)).astype(jnp.int32)
            stats[0:8, :] = jnp.zeros((SUBLANES, LANES), jnp.float32)
            stats[8:16, :] = 1.0 / (1.0 - int_power(0.9, steps))
            stats[16:24, :] = 1.0 / (1.0 - int_power(0.999, steps))
        copy = pltpu.make_async_remote_copy(
            recv, recv, row_sent, a_sem.at[stage], device_id=sibling, device_id_type=MESH
        )
        with jax.named_scope("norm_wait"):
            copy.wait_recv()
        copy.wait_send()
        chains = [jnp.concatenate(result, axis=0)] + [recv[i] for i in range(min(3, recv.shape[0]))]
        for i in range(3, len(offsets_of(axes))):
            chains[i % 4] = chains[i % 4] + recv[i]
        both = functools.reduce(jnp.add, chains[:1 + len(offsets_of(axes))])
        result = [both[0:1], both[1:2]]
    for i, row in enumerate(result):
        stats[i:i + 1, :] = row

    with jax.named_scope("send_wait"):
        pltpu.make_async_remote_copy(
            pair_send.at[0], pair_recv.at[0], pair_sent, pr_sem.at[0], device_id=sibling, device_id_type=MESH
        ).wait_send()
        if far:
            pltpu.make_async_remote_copy(
                ring_send.at[slots, sent], ring_recv.at[slots, sent], ring_sent, rr_sem.at[0, 0],
                device_id=sibling, device_id_type=MESH,
            ).wait_send()
        if relayed:
            @pl.when(core == 0)
            def _():
                tail_pair().wait_send()

            @pl.when(core == 1)
            def _():
                pltpu.make_async_remote_copy(
                    tail_ring, tail_recv, tail_sent, tail_sem.at[0], device_id=sibling, device_id_type=MESH
                ).wait_send()

            for h, taken in enumerate(borrow):
                @pl.when(taken)
                def _():
                    forward_copy(h).wait_send()


def update(
    entries, chunks, stats, grad_ref, held,
    w_out, m_out, v_out, dir_out, drop_out, bufs, drop_ref, sems,
):
    rows, width = grad_ref.shape
    part = rows // chunks
    scale_m = jnp.concatenate([stats[8:16, :]] * (width // LANES), axis=1)
    scale_v = jnp.concatenate([stats[16:24, :]] * (width // LANES), axis=1)
    summed = jnp.sum(jnp.broadcast_to(stats[0:1, :], (SUBLANES, LANES)), axis=1, keepdims=True)
    rms = jnp.sqrt(summed * (1.0 / entries))
    clip = jnp.minimum(1.0, 0.05 / (rms + 1e-06))
    share_m, share_v = 0.1 * clip, math.sqrt(0.001) * clip
    outs = (w_out, m_out, v_out, dir_out)

    def put(i, k, value):
        bufs[i, k * part:(k + 1) * part, :] = value
        rows_of = pl.ds(k * part, part)
        pltpu.make_async_copy(bufs.at[i, rows_of], outs[i].at[0, 0, rows_of], sems.at[i]).start()

    for k in range(chunks):
        at = slice(k * part, (k + 1) * part)
        grad = grad_ref[at, :]
        root = grad * share_v
        put(1, k, held[1, at, :] + grad * share_m)
        put(2, k, held[2, at, :] + root * root)
    for k in range(chunks):
        at = slice(k * part, (k + 1) * part)
        weights = held[0, at, :]
        corrected = bufs[2, at, :] * scale_v
        direction = (bufs[1, at, :] * scale_m) / (corrected * lax.rsqrt(corrected) + 1e-08) + 0.1 * weights
        put(3, k, direction)
        put(0, k, weights - 0.001 * direction)
        if k == 0:
            drop_ref[0] = jnp.max(stats[1:2, :]).astype(jnp.int32)
            drop = pltpu.make_async_copy(drop_ref, drop_out, sems.at[4])
            drop.start()
    for i, out in enumerate(outs):
        pltpu.make_async_copy(bufs.at[i], out.at[0, 0], sems.at[i]).wait()
    drop.wait()


def body(sizes, grad_parts, drop_flags, owner_order, step_count, master, moment_m, moment_v):
    n = sizes["dp"]
    chips = n // 2
    rows, columns = grad_parts.shape[-2:]
    width = master.shape[-1]
    chunks = rows // 8
    cuts = sorted({0, 8, rows - 24, rows - 8, rows})
    devices = n * sizes["tensor"] * sizes["pipe"]
    stages = [AXES] if devices <= DIRECT else [(axis,) for axis in AXES]
    peers = []
    for axes in stages:
        size = 1
        for axis in axes:
            size *= sizes[axis]
        peers.append(size - 1)
    entries = rows * columns * sizes["tensor"] * sizes["pipe"]
    padded = -(-rows // LANES) * LANES
    others = max(chips - 1, 1)
    rounds = max(sizes["pipe"] - 2, 0) + sizes["tensor"]
    f32 = jnp.float32
    dma = pltpu.SemaphoreType.DMA
    vmem = pl.BlockSpec(memory_space=pltpu.VMEM)
    hbm = pl.BlockSpec(memory_space=pltpu.HBM)
    state = jax.ShapeDtypeStruct(master.shape, f32)
    block = rows * columns * 4
    inputs = (owner_order, drop_flags.reshape(drop_flags.shape[-3:]), grad_parts, master, moment_m, moment_v)
    steps = lax.cond(
        lax.axis_index(stages[0]) == 0,
        lambda count: jnp.full((2, LANES), count.astype(f32)),
        lambda count: jnp.zeros((2, LANES), f32),
        step_count,
    )
    total, held, stats = pl.pallas_call(
        functools.partial(exchange, sizes, stages, cuts),
        out_shape=tuple(pltpu.VMEM(shape, f32) for shape in ((rows, width), (3, rows, width), (3 * SUBLANES, LANES))),
        in_specs=[vmem] + [hbm] * 6,
        out_specs=(vmem,) * 3,
        scratch_shapes=[
            pltpu.SMEM((n,), jnp.int32),
            pltpu.VMEM((1, 1, rows), jnp.int32),
            [pltpu.VMEM((n, end - start, width), f32) for start, end in zip(cuts, cuts[1:])],
            pltpu.VMEM((chips, rows, width), f32),
            pltpu.VMEM((chips, rows, width), f32),
            pltpu.VMEM((others, rows, width), f32),
            pltpu.VMEM((others, rows, width), f32),
            pltpu.VMEM((1, 1, padded), f32),
            pltpu.VMEM((n - 1, 1, padded), f32),
            [pltpu.VMEM((2, LANES), f32) for _ in peers],
            [pltpu.VMEM((max(size, 1), 2, LANES), f32) for size in peers],
            pltpu.VMEM((2, LANES), f32),
            pltpu.VMEM((2, LANES), f32),
            pltpu.VMEM((PIECES - 1, 16, width // 2), f32),
            pltpu.VMEM((2, 8, width), f32),
            pltpu.VMEM((2, 8, width), f32),
            pltpu.VMEM((2, 8, width), f32),
            dma((2,)),
            dma((max(len(cuts) - 1, 4),)),
            dma((len(cuts) - 1 if can_relay(sizes, stages) else len(cuts),)),
            dma((len(cuts) - 1, others)),
            dma((1,)),
            dma((len(peers),)),
            dma((PIECES - 1,)),
            dma((1,)),
            dma((1,)),
            pltpu.SemaphoreType.REGULAR((3,)),
            pltpu.SemaphoreType.REGULAR((rounds,)),
        ],
        compiler_params=pltpu.CompilerParams(
            collective_id=0, has_side_effects=True, vmem_limit_bytes=8 * block
        ),
        cost_estimate=pl.CostEstimate(
            flops=8 * rows * columns, bytes_accessed=20 * rows * columns * 4, transcendentals=0
        ),
    )(pltpu.with_memory_space_constraint(steps, pltpu.VMEM), *(pltpu.with_memory_space_constraint(x, pltpu.HBM) for x in inputs))
    outs = pl.pallas_call(
        functools.partial(update, entries, chunks),
        out_shape=(state, state, state, state, jax.ShapeDtypeStruct((1,), jnp.int32)),
        in_specs=[vmem] * 3,
        out_specs=(hbm,) * 5,
        scratch_shapes=[pltpu.VMEM((4, rows, width), f32), pltpu.SMEM((1,), jnp.int32), dma((5,))],
        compiler_params=pltpu.CompilerParams(vmem_limit_bytes=8 * block),
        cost_estimate=pl.CostEstimate(
            flops=20 * rows * width, bytes_accessed=8 * rows * width * 4, transcendentals=0
        ),
    )(stats, total, held)
    return (*outs[:4], outs[4].reshape(()))


def solution(mesh):
    return jax.shard_map(
        functools.partial(body, dict(mesh.shape)),
        mesh=mesh,
        in_specs=(
            P("dp", "pipe", "tensor", None, None),
            P("dp", "pipe", "tensor", None),
            P(),
            P(),
            P("pipe", "tensor", None, "dp"),
            P("pipe", "tensor", None, "dp"),
            P("pipe", "tensor", None, "dp"),
        ),
        out_specs=(
            P("pipe", "tensor", None, "dp"),
            P("pipe", "tensor", None, "dp"),
            P("pipe", "tensor", None, "dp"),
            P("pipe", "tensor", None, "dp"),
            P(),
        ),
        check_vma=False,
    )
```

```python
import functools
import itertools
import math
import jax
import jax.numpy as jnp
from jax import lax
from jax.experimental import pallas as pl
from jax.experimental.pallas import tpu as pltpu
from jax.sharding import PartitionSpec as P

AXES = ("dp", "tensor", "pipe")
MESH = pl.DeviceIdType.MESH
LANES = 128
SUBLANES = 8
DIRECT = 64
EDGES = (0, 3, 8, 11, 16)
PIECES = len(EDGES) - 1


def as_column(row, rows):
    square = (rows, rows)
    diagonal = lax.broadcasted_iota(jnp.int32, square, 0) == lax.broadcasted_iota(jnp.int32, square, 1)
    return jnp.sum(jnp.where(diagonal, jnp.broadcast_to(row, square), 0.0), axis=1, keepdims=True)


def int_power(base, exponent):
    result = jnp.ones(exponent.shape, jnp.float32)
    square = jnp.full(exponent.shape, base, jnp.float32)
    for bit in range(31):
        result = jnp.where((exponent >> bit) & 1 == 1, result * square, result)
        square = square * square
    return result


def can_relay(sizes, stages):
    return sizes["dp"] == 4 and sizes["tensor"] == 2 and len(stages) == 1 and sizes["pipe"] > 1


def exchange(
    sizes, stages, cuts,
    step_ref, order_hbm, flags_hbm, grad_hbm, w_hbm, m_hbm, v_hbm,
    total, held, stats,
    order_ref, flags_ref, g_bufs, pair_send, pair_recv, ring_send, ring_recv,
    kept_send, kept_recv, red_sends, red_recvs,
    step_send, step_recv, relay_buf, tail_send, tail_recv, tail_ring,
    o_sem, g_sem, pr_sem, rr_sem, k_sem, a_sem, via_sem, step_sem, tail_sem, chain_sem, ready_sem,
):
    n = sizes["dp"]
    chips = n // 2
    relayed = can_relay(sizes, stages)
    rows, width = total.shape
    parts = [(start, end - start) for start, end in zip(cuts, cuts[1:])]
    me = {axis: lax.axis_index(axis) for axis in AXES}
    chip, core = lax.div(me["dp"], 2), lax.rem(me["dp"], 2)

    def peer(offsets):
        return {axis: lax.rem(me[axis] + off, sizes[axis]) for axis, off in offsets.items()}

    def offsets_of(axes):
        ranges = [range(sizes[axis]) for axis in axes]
        return [dict(zip(axes, offs)) for offs in itertools.product(*ranges) if any(offs)]

    pair_sent, row_sent = o_sem.at[0], o_sem.at[1]
    ring_sent, tail_sent, held_sem, tail_paired = (g_sem.at[i] for i in range(4))
    small = [
        pltpu.make_async_copy(flags_hbm, flags_ref, o_sem.at[0]),
        pltpu.make_async_copy(order_hbm, order_ref, o_sem.at[1]),
    ]
    for copy in small:
        copy.start()
    loads = []

    def load(k):
        start, size = parts[k]
        for b in range(n):
            pltpu.make_async_copy(
                grad_hbm.at[0, 0, 0, pl.ds(start, size), pl.ds(b * width, width)], g_bufs[k].at[b], g_sem.at[k]
            ).start()
        loads.append(pltpu.make_async_copy(g_bufs[k], g_bufs[k], g_sem.at[k]))

    load(0)

    def greet(sem, axis):
        if axis == "dp":
            for off in range(1, n):
                pl.semaphore_signal(sem, inc=1, device_id=peer({"dp": off}), device_id_type=MESH)
            return n - 1
        at, last = me[axis], sizes[axis] - 1

        @pl.when(at > 0)
        def _():
            pl.semaphore_signal(sem, inc=1, device_id={**home, axis: at - 1}, device_id_type=MESH)

        @pl.when(at < last)
        def _():
            pl.semaphore_signal(sem, inc=1, device_id={**home, axis: at + 1}, device_id_type=MESH)

        return jnp.minimum(at, 1) + jnp.minimum(last - at, 1)

    sibling = {"dp": chip * 2 + 1 - core}
    barrier = pltpu.get_barrier_semaphore()

    @pl.when(core == 1)
    def _():
        pl.semaphore_signal(barrier, inc=1, device_id=sibling, device_id_type=MESH)

    home = {"dp": chip * 2 + 1}
    for off in range(1, chips):
        pl.semaphore_signal(
            barrier, inc=1, device_id={"dp": lax.rem(chip + off, chips) * 2 + 1}, device_id_type=MESH
        )
    met = 2 * (chips - 1 + greet(barrier, "tensor") + greet(barrier, "pipe"))
    home = {}
    rounds = ["pipe"] * max(sizes["pipe"] - 2, 0) + ["tensor"] * (sizes["tensor"] - 1) + ["dp"]
    left, owed = list(rounds), []

    def next_round():
        if owed:
            at, amount = owed.pop()
            pl.semaphore_wait(ready_sem.at[at], amount)
        if left:
            at = len(rounds) - len(left)
            owed.append((at, greet(ready_sem.at[at], left.pop(0))))

    load(1)

    @pl.when(core == 0)
    def _():
        pl.semaphore_wait(barrier, 1)
        pl.semaphore_signal(chain_sem.at[2], inc=1, device_id=sibling, device_id_type=MESH)

    for copy in small:
        copy.wait()
    for k in range(2, len(parts)):
        load(k)
    flags_row = flags_ref[0].astype(jnp.float32)
    kept_row = 1.0 - flags_row
    kept = as_column(kept_row, rows)
    kept_send[0, :, 0:rows] = kept_row
    dropped = jnp.sum(flags_row, axis=1, keepdims=True)

    def chip_at(slot):
        return lax.rem(chip + slot, chips)

    def term(k, owner):
        start, size = parts[k]
        return g_bufs[k][order_ref[owner]] * kept[start:start + size]

    def rows_of(ref, slot, k):
        start, size = parts[k]
        return ref.at[slot, pl.ds(start, size)]

    pair = {}

    def send_pair(k, slot):
        copy = pltpu.make_async_remote_copy(
            rows_of(pair_send, slot, k), rows_of(pair_recv, slot, k),
            pair_sent, pr_sem.at[k if slot else pr_sem.shape[0] - 1],
            device_id=sibling, device_id_type=MESH,
        )
        copy.start()
        pair[k, slot] = copy

    far = list(range(1, chips))
    def to_sibling(k):
        start, size = parts[k]
        with jax.named_scope(f"load_wait{k}"):
            loads[k].wait()
        for slot in far:
            pair_send[slot, start:start + size, :] = term(k, chip_at(slot) * 2 + 1 - core)
        if k == 0:
            with jax.named_scope("sibling_wait"):
                @pl.when(core == 1)
                def _():
                    pl.semaphore_wait(chain_sem.at[2], 1)
        for slot in far:
            send_pair(k, slot)

    kepts = pltpu.make_async_remote_copy(
        kept_recv, kept_recv, row_sent, k_sem.at[0], device_id=sibling, device_id_type=MESH
    )

    ring = {}
    swing = len(parts) - 2
    far_end = sizes["pipe"] - 1
    gap = 2 * me["pipe"] - far_end
    across = {"dp": chip_at(1) * 2 + core}
    lend = [gap >= 1, gap >= 3, 2 * me["tensor"] >= sizes["tensor"]] if relayed else []
    borrow = [gap <= -1, gap <= -3, 2 * me["tensor"] < sizes["tensor"]] if relayed else []
    mirror = [{"pipe": far_end - me["pipe"]}] * 2 + [{"tensor": sizes["tensor"] - 1 - me["tensor"]}]
    edges = [width * edge // 16 for edge in EDGES]

    def piece(ref, h):
        start, size = parts[swing]
        return ref.at[0, pl.ds(start, size), pl.ds(edges[h], edges[h + 1] - edges[h])]

    def lodging(h):
        return relay_buf.at[h, :, pl.ds(0, edges[h + 1] - edges[h])]

    def swing_copy(h):
        return pltpu.make_async_remote_copy(
            piece(ring_send, h), piece(ring_recv, h), ring_sent, rr_sem.at[swing, 0],
            device_id=across, device_id_type=MESH,
        )

    def via_copy(h):
        return pltpu.make_async_remote_copy(
            piece(ring_send, h), lodging(h), ring_sent, via_sem.at[h],
            device_id={**across, **mirror[h]}, device_id_type=MESH,
        )

    def forward_copy(h):
        return pltpu.make_async_remote_copy(
            lodging(h), piece(ring_recv, h), via_sem.at[h], rr_sem.at[swing, 0],
            device_id=mirror[h], device_id_type=MESH,
        )

    def climb():
        at = me["pipe"]

        @pl.when(at >= 2)
        def _():
            pl.semaphore_wait(chain_sem.at[0], 1)

        @pl.when((at >= 1) & (at < far_end))
        def _():
            pl.semaphore_signal(chain_sem.at[0], inc=1, device_id={"pipe": at + 1}, device_id_type=MESH)

        @pl.when(lend[0] | lend[2])
        def _():
            pl.semaphore_signal(chain_sem.at[1], inc=1, device_id=across, device_id_type=MESH)

    tail = len(parts) - 1
    tail_at = pl.ds(*parts[tail])
    abroad = chip_at(1) * 2

    def tail_pair():
        return pltpu.make_async_remote_copy(
            tail_send, tail_recv, tail_paired, tail_sem.at[0], device_id=sibling, device_id_type=MESH
        )

    def tail_copy(c):
        return pltpu.make_async_remote_copy(
            tail_ring.at[c], ring_recv.at[0, tail_at], tail_sent, rr_sem.at[tail, 0],
            device_id={"dp": abroad + c}, device_id_type=MESH,
        )

    def tail_to_sibling():
        loads[tail].wait()

        @pl.when(core == 0)
        def _():
            for c in range(2):
                tail_send[c] = term(tail, abroad + c)
            tail_pair().start()

    def tail_to_owner():
        @pl.when(core == 1)
        def _():
            tail_pair().wait_recv()
            for c in range(2):
                tail_ring[c] = tail_recv[c] + term(tail, abroad + c)
                tail_copy(c).start()

    def to_owner(k):
        start, size = parts[k]
        for slot in far:
            target = chip_at(slot) * 2 + core
            mine = term(k, target)
            with jax.named_scope(f"pair_wait{k}"):
                if slot == far[0]:
                    pltpu.make_async_remote_copy(
                        pair_recv.at[pl.ds(1, chips - 1), pl.ds(start, size)],
                        pair_recv.at[pl.ds(1, chips - 1), pl.ds(start, size)],
                        pair_sent, pr_sem.at[k], device_id=sibling, device_id_type=MESH,
                    ).wait_recv()
            ring_send[slot - 1, start:start + size, :] = pair_recv[slot, start:start + size, :] + mine
            if relayed and k == swing:
                @pl.when(lend[0] | lend[2])
                def _():
                    with jax.named_scope("chain_wait"):
                        pl.semaphore_wait(chain_sem.at[1], 1)

                for h, away in ((1, lend[1]), (0, lend[0]), (2, lend[2])):
                    @pl.when(away)
                    def _():
                        via_copy(h).start()

                for h, away in enumerate(lend):
                    @pl.when(jnp.logical_not(away))
                    def _():
                        swing_copy(h).start()
                for h in range(len(lend), PIECES):
                    swing_copy(h).start()
                continue
            copy = pltpu.make_async_remote_copy(
                rows_of(ring_send, slot - 1, k), rows_of(ring_recv, slot - 1, k),
                ring_sent, rr_sem.at[k, slot - 1],
                device_id={"dp": target}, device_id_type=MESH,
            )
            copy.start()
            ring[k, slot] = copy

    to_sibling(0)
    to_sibling(1)
    with jax.named_scope("barrier_wait"):
        @pl.when(core == 1)
        def _():
            pl.semaphore_wait(barrier, met)
            pl.semaphore_signal(chain_sem.at[2], inc=1, device_id=sibling, device_id_type=MESH)

        @pl.when(core == 0)
        def _():
            pl.semaphore_wait(chain_sem.at[2], 1)
    for off in range(1, n):
        pltpu.make_async_remote_copy(
            kept_send.at[0], kept_recv.at[off - 1], row_sent, k_sem.at[0],
            device_id=peer({"dp": off}), device_id_type=MESH,
        ).start()
    to_owner(0)
    if relayed:
        climb()
    else:
        to_owner(1)
    if relayed:
        to_sibling(swing)
        tail_to_sibling()
        to_owner(1)
        tail_to_owner()
        to_owner(swing)
    else:
        for k in range(2, len(parts)):
            to_sibling(k)
        for k in range(2, len(parts)):
            to_owner(k)

    next_round()
    sent = pl.ds(0, parts[tail][0] if relayed else rows)
    slots = pl.ds(0, chips - 1)
    if far:
        pltpu.make_async_remote_copy(
            ring_send.at[slots, sent], ring_recv.at[slots, sent], pair_sent, pr_sem.at[0],
            device_id=sibling, device_id_type=MESH,
        ).wait_send()
    for k, (start, size) in enumerate(parts):
        pair_send[0, start:start + size, :] = term(k, chip * 2 + 1 - core)
        send_pair(k, 0)
    with jax.named_scope("kept_wait"):
        kepts.wait_recv()
    kepts.wait_send()
    count_row = kept_row
    for i in range(n - 1):
        count_row = count_row + kept_recv[i, :, 0:rows]
    inverse = 1.0 / jnp.maximum(as_column(count_row, rows), 1.0)
    next_round()
    for i, source in enumerate((w_hbm, m_hbm, v_hbm)):
        pltpu.make_async_copy(source.at[0, 0], held.at[i], held_sem).start()

    pltpu.make_async_remote_copy(
        pair_recv.at[0], pair_recv.at[0], pair_sent, pr_sem.at[pr_sem.shape[0] - 1],
        device_id=sibling, device_id_type=MESH,
    ).wait_recv()
    for k, (start, size) in enumerate(parts):
        total[start:start + size, :] = pair_recv[0, start:start + size, :] + term(k, me["dp"])
    pltpu.make_async_copy(held, held, held_sem).wait()
    held[1] = 0.9 * held[1]
    held[2] = 0.999 * held[2]
    next_round()

    if relayed:
        for h in (2, 1, 0):
            @pl.when(borrow[h])
            def _():
                with jax.named_scope(f"relay_wait{h}"):
                    via_copy(h).wait_recv()
                forward_copy(h).start()

    while left or owed:
        next_round()
    first = functools.reduce(jnp.logical_and, [me[axis] == 0 for axis in stages[0]])

    def tell(device):
        return pltpu.make_async_remote_copy(
            step_send, step_recv, row_sent, step_sem.at[0], device_id=device, device_id_type=MESH
        )

    @pl.when(first)
    def _():
        step_send[...] = step_ref[...]
        step_recv[...] = step_ref[...]
        for off in offsets_of(stages[0]):
            tell(off).start()

    squares = jnp.zeros((SUBLANES, LANES), jnp.float32)
    for k in [i for i in range(len(parts)) if not relayed or i != swing] + [swing] * relayed:
        start, size = parts[k]
        at = slice(start, start + size)
        value = total[at, :]
        for slot in far:
            with jax.named_scope(f"ring_wait{k}"):
                if relayed and k == swing:
                    pltpu.make_async_remote_copy(
                        ring_recv.at[0, pl.ds(start, size)], ring_recv.at[0, pl.ds(start, size)],
                        ring_sent, rr_sem.at[swing, 0], device_id=across, device_id_type=MESH,
                    ).wait_recv()
                elif relayed and k == tail:
                    tail_copy(0).wait_recv()
                else:
                    ring[k, slot].wait_recv()
            value = value + ring_recv[slot - 1, at, :]
        value = value * inverse[at]
        total[at, :] = value
        squares = squares + jnp.sum(
            (value * value).reshape(size // SUBLANES, SUBLANES, width // LANES, LANES), axis=(0, 2)
        )

    @pl.when(first)
    def _():
        pltpu.make_async_remote_copy(
            red_recvs[0], red_recvs[0], row_sent, step_sem.at[0], device_id=sibling, device_id_type=MESH
        ).wait_send()

    result = [jnp.sum(squares, axis=0, keepdims=True), jnp.broadcast_to(dropped, (1, LANES))]
    for stage, (axes, send, recv) in enumerate(zip(stages, red_sends, red_recvs)):
        for i, row in enumerate(result):
            send[i:i + 1, :] = row
        with jax.named_scope("norm_send"):
            back, stride = 0, 1
            for axis in reversed(axes):
                back, stride = back + lax.rem(sizes[axis] - me[axis], sizes[axis]) * stride, stride * sizes[axis]

            def share(i, device):
                pltpu.make_async_remote_copy(
                    send, recv.at[i], row_sent, a_sem.at[stage],
                    device_id=device, device_id_type=MESH,
                ).start()

            @pl.when(back > 0)
            def _():
                share(back - 1, dict.fromkeys(axes, 0))

            for i, off in enumerate(offsets_of(axes)):
                @pl.when(back != i + 1)
                def _():
                    share(i, peer(off))
        if stage == 0:
            @pl.when(jnp.logical_not(first))
            def _():
                tell(sibling).wait_recv()

            steps = jnp.broadcast_to(step_recv[0:1, :], (SUBLANES, LANES)).astype(jnp.int32)
            stats[0:8, :] = jnp.zeros((SUBLANES, LANES), jnp.float32)
            stats[8:16, :] = 1.0 / (1.0 - int_power(0.9, steps))
            stats[16:24, :] = 1.0 / (1.0 - int_power(0.999, steps))
        copy = pltpu.make_async_remote_copy(
            recv, recv, row_sent, a_sem.at[stage], device_id=sibling, device_id_type=MESH
        )
        with jax.named_scope("norm_wait"):
            copy.wait_recv()
        copy.wait_send()
        chains = [jnp.concatenate(result, axis=0)] + [recv[i] for i in range(min(3, recv.shape[0]))]
        for i in range(3, len(offsets_of(axes))):
            chains[i % 4] = chains[i % 4] + recv[i]
        both = functools.reduce(jnp.add, chains[:1 + len(offsets_of(axes))])
        result = [both[0:1], both[1:2]]
    for i, row in enumerate(result):
        stats[i:i + 1, :] = row

    with jax.named_scope("send_wait"):
        pltpu.make_async_remote_copy(
            pair_send.at[0], pair_recv.at[0], pair_sent, pr_sem.at[0], device_id=sibling, device_id_type=MESH
        ).wait_send()
        if far:
            pltpu.make_async_remote_copy(
                ring_send.at[slots, sent], ring_recv.at[slots, sent], ring_sent, rr_sem.at[0, 0],
                device_id=sibling, device_id_type=MESH,
            ).wait_send()
        if relayed:
            @pl.when(core == 0)
            def _():
                tail_pair().wait_send()

            @pl.when(core == 1)
            def _():
                pltpu.make_async_remote_copy(
                    tail_ring, tail_recv, tail_sent, tail_sem.at[0], device_id=sibling, device_id_type=MESH
                ).wait_send()

            for h, taken in enumerate(borrow):
                @pl.when(taken)
                def _():
                    forward_copy(h).wait_send()


def update(
    entries, chunks, stats, grad_ref, held,
    w_out, m_out, v_out, dir_out, drop_out, bufs, drop_ref, sems,
):
    rows, width = grad_ref.shape
    part = rows // chunks
    scale_m = jnp.concatenate([stats[8:16, :]] * (width // LANES), axis=1)
    scale_v = jnp.concatenate([stats[16:24, :]] * (width // LANES), axis=1)
    summed = jnp.sum(jnp.broadcast_to(stats[0:1, :], (SUBLANES, LANES)), axis=1, keepdims=True)
    rms = jnp.sqrt(summed * (1.0 / entries))
    clip = jnp.minimum(1.0, 0.05 / (rms + 1e-06))
    share_m, share_v = 0.1 * clip, math.sqrt(0.001) * clip
    outs = (w_out, m_out, v_out, dir_out)

    def put(i, k, value):
        bufs[i, k * part:(k + 1) * part, :] = value
        rows_of = pl.ds(k * part, part)
        pltpu.make_async_copy(bufs.at[i, rows_of], outs[i].at[0, 0, rows_of], sems.at[i]).start()

    for k in range(chunks):
        at = slice(k * part, (k + 1) * part)
        grad = grad_ref[at, :]
        root = grad * share_v
        put(1, k, held[1, at, :] + grad * share_m)
        put(2, k, held[2, at, :] + root * root)
    for k in range(chunks):
        at = slice(k * part, (k + 1) * part)
        weights = held[0, at, :]
        corrected = bufs[2, at, :] * scale_v
        direction = (bufs[1, at, :] * scale_m) / (corrected * lax.rsqrt(corrected) + 1e-08) + 0.1 * weights
        put(3, k, direction)
        put(0, k, weights - 0.001 * direction)
        if k == 0:
            drop_ref[0] = jnp.max(stats[1:2, :]).astype(jnp.int32)
            drop = pltpu.make_async_copy(drop_ref, drop_out, sems.at[4])
            drop.start()
    for i, out in enumerate(outs):
        pltpu.make_async_copy(bufs.at[i], out.at[0, 0], sems.at[i]).wait()
    drop.wait()


def body(sizes, grad_parts, drop_flags, owner_order, step_count, master, moment_m, moment_v):
    n = sizes["dp"]
    chips = n // 2
    rows, columns = grad_parts.shape[-2:]
    width = master.shape[-1]
    chunks = rows // 8
    cuts = sorted({0, 8, rows - 24, rows - 8, rows})
    devices = n * sizes["tensor"] * sizes["pipe"]
    stages = [AXES] if devices <= DIRECT else [(axis,) for axis in AXES]
    peers = []
    for axes in stages:
        size = 1
        for axis in axes:
            size *= sizes[axis]
        peers.append(size - 1)
    entries = rows * columns * sizes["tensor"] * sizes["pipe"]
    padded = -(-rows // LANES) * LANES
    others = max(chips - 1, 1)
    rounds = max(sizes["pipe"] - 2, 0) + sizes["tensor"]
    f32 = jnp.float32
    dma = pltpu.SemaphoreType.DMA
    vmem = pl.BlockSpec(memory_space=pltpu.VMEM)
    hbm = pl.BlockSpec(memory_space=pltpu.HBM)
    state = jax.ShapeDtypeStruct(master.shape, f32)
    block = rows * columns * 4
    inputs = (owner_order, drop_flags.reshape(drop_flags.shape[-3:]), grad_parts, master, moment_m, moment_v)
    steps = lax.cond(
        lax.axis_index(stages[0]) == 0,
        lambda count: jnp.full((2, LANES), count.astype(f32)),
        lambda count: jnp.zeros((2, LANES), f32),
        step_count,
    )
    total, held, stats = pl.pallas_call(
        functools.partial(exchange, sizes, stages, cuts),
        out_shape=tuple(pltpu.VMEM(shape, f32) for shape in ((rows, width), (3, rows, width), (3 * SUBLANES, LANES))),
        in_specs=[vmem] + [hbm] * 6,
        out_specs=(vmem,) * 3,
        scratch_shapes=[
            pltpu.SMEM((n,), jnp.int32),
            pltpu.VMEM((1, 1, rows), jnp.int32),
            [pltpu.VMEM((n, end - start, width), f32) for start, end in zip(cuts, cuts[1:])],
            pltpu.VMEM((chips, rows, width), f32),
            pltpu.VMEM((chips, rows, width), f32),
            pltpu.VMEM((others, rows, width), f32),
            pltpu.VMEM((others, rows, width), f32),
            pltpu.VMEM((1, 1, padded), f32),
            pltpu.VMEM((n - 1, 1, padded), f32),
            [pltpu.VMEM((2, LANES), f32) for _ in peers],
            [pltpu.VMEM((max(size, 1), 2, LANES), f32) for size in peers],
            pltpu.VMEM((2, LANES), f32),
            pltpu.VMEM((2, LANES), f32),
            pltpu.VMEM((PIECES - 1, 16, width // 2), f32),
            pltpu.VMEM((2, 8, width), f32),
            pltpu.VMEM((2, 8, width), f32),
            pltpu.VMEM((2, 8, width), f32),
            dma((2,)),
            dma((max(len(cuts) - 1, 4),)),
            dma((len(cuts) - 1 if can_relay(sizes, stages) else len(cuts),)),
            dma((len(cuts) - 1, others)),
            dma((1,)),
            dma((len(peers),)),
            dma((PIECES - 1,)),
            dma((1,)),
            dma((1,)),
            pltpu.SemaphoreType.REGULAR((3,)),
            pltpu.SemaphoreType.REGULAR((rounds,)),
        ],
        compiler_params=pltpu.CompilerParams(
            collective_id=0, has_side_effects=True, vmem_limit_bytes=8 * block
        ),
        cost_estimate=pl.CostEstimate(
            flops=8 * rows * columns, bytes_accessed=20 * rows * columns * 4, transcendentals=0
        ),
    )(pltpu.with_memory_space_constraint(steps, pltpu.VMEM), *(pltpu.with_memory_space_constraint(x, pltpu.HBM) for x in inputs))
    outs = pl.pallas_call(
        functools.partial(update, entries, chunks),
        out_shape=(state, state, state, state, jax.ShapeDtypeStruct((1,), jnp.int32)),
        in_specs=[vmem] * 3,
        out_specs=(hbm,) * 5,
        scratch_shapes=[pltpu.VMEM((4, rows, width), f32), pltpu.SMEM((1,), jnp.int32), dma((5,))],
        compiler_params=pltpu.CompilerParams(vmem_limit_bytes=8 * block),
        cost_estimate=pl.CostEstimate(
            flops=20 * rows * width, bytes_accessed=8 * rows * width * 4, transcendentals=0
        ),
    )(stats, total, held)
    return (*outs[:4], outs[4].reshape(()))


def solution(mesh):
    return jax.shard_map(
        functools.partial(body, dict(mesh.shape)),
        mesh=mesh,
        in_specs=(
            P("dp", "pipe", "tensor", None, None),
            P("dp", "pipe", "tensor", None),
            P(),
            P(),
            P("pipe", "tensor", None, "dp"),
            P("pipe", "tensor", None, "dp"),
            P("pipe", "tensor", None, "dp"),
        ),
        out_specs=(
            P("pipe", "tensor", None, "dp"),
            P("pipe", "tensor", None, "dp"),
            P("pipe", "tensor", None, "dp"),
            P("pipe", "tensor", None, "dp"),
            P(),
        ),
        check_vma=False,
    )
```
